128 devices in a mesh: group: 8 (over y, core), peer: 16 (over z, x).
Axes of the slice: x: 4, y: 4, z: 4, core: 2. Of those that a mesh axis runs over, the one named last changes fastest.
Arguments:
- states: float32 [41, 4194304], P(None, ('group', 'peer')), may hold values from -6 to 6
- block_part: int32 [32768], P(('group', 'peer')), may hold values from 0 to 127, as said below
- tile_perm: int32 [32768, 128], P(('group', 'peer')), may hold values from 0 to 127, each once within a row
- half_volt: float32 [40], replicated, may hold values from -4 to 4
- steepness: float32 [40], replicated, may hold values from 0.5 to 4
- gate_rate: float32 [40], replicated, may hold values from 0.1 to 1
- conductance: float32 [40], replicated, may hold values from 0.005 to 0.08
- reversal: float32 [40], replicated, may hold values from -6 to 6
Outputs:
- regrouped: float32 [41, 4194304], P(None, ('group', 'peer'))
The draws below stay inside these ranges and needn't reach their ends.
Inputs may be any that keep to these rules, and one draw needn't show every extreme that they name: `block_part`: every partition holds exactly 256 blocks. Within each slab of 256 consecutive global blocks no partition holds more than 4 blocks; every slab has exactly 4 blocks of some partition, and every partition has exactly 4 blocks in some slab.
All inputs are finite; a program needn't handle non-finite values.
Results may differ from the reference program's by a relative error of at most 0.0001.
Values sent between devices are 32-bit elements; how exact they have to be, the bound alone decides.
A program may use at most 192 MiB of HBM per device.

```python
import math
import jax
import jax.numpy as jnp
from jax import lax

STATES = 41
NODE_BLK = 128
BLK_DEV = 256
SUBSTEPS = 1
GATES = 40
BLOCKS = 32768
NODES = 4194304


def draw_block_part(key, part):
    devices = BLOCKS // BLK_DEV
    mean_count = BLK_DEV // devices
    pair_count = devices // 2
    key_order = jax.random.fold_in(key, 11)
    key_amount = jax.random.fold_in(key, 12)
    key_shuffle = jax.random.fold_in(key, 13)
    ordering = jax.random.permutation(key_order, devices).astype(jnp.int32)
    amounts = jax.random.randint(key_amount, (pair_count,), -mean_count, mean_count + 1, dtype=jnp.int32)
    amounts = amounts.at[0].set(mean_count)
    row_ids = jnp.arange(devices, dtype=jnp.int32)
    pair_ids = jnp.arange(pair_count, dtype=jnp.int32)
    plus_cols = ordering[(row_ids[:, None] + 2 * pair_ids[None, :]) % devices]
    minus_cols = ordering[(row_ids[:, None] + 2 * pair_ids[None, :] + 1) % devices]
    row_grid = jnp.broadcast_to(row_ids[:, None], (devices, pair_count))
    amount_grid = jnp.broadcast_to(amounts[None, :], (devices, pair_count))
    counts = jnp.full((devices, devices), mean_count, jnp.int32)
    counts = counts.at[row_grid, plus_cols].add(amount_grid)
    counts = counts.at[row_grid, minus_cols].add(-amount_grid)
    running = jnp.cumsum(counts, axis=1, dtype=jnp.int32)
    position = jnp.arange(BLK_DEV, dtype=jnp.int32)
    labels = jnp.sum((running[:, None, :] <= position[None, :, None]).astype(jnp.int32), axis=2, dtype=jnp.int32)
    row_keys = jax.random.split(key_shuffle, devices)
    shuffled = jax.vmap(lambda row_key, row_vals: jax.random.permutation(row_key, row_vals))(row_keys, labels)
    return shuffled.reshape(-1).astype(jnp.int32)


def level_of(own_key, extent, cuts, low, largest):
    gain = 1.0
    for dim, parts in cuts:
        steps = jax.random.uniform(jax.random.fold_in(jax.random.fold_in(own_key, 6), dim), (parts,), jnp.float32, low / len(cuts), largest / len(cuts))
        gain = gain * jnp.repeat(jnp.exp(steps), extent[dim] // parts).reshape((-1,) + (1,) * (len(extent) - 1 - dim))
    return gain


def normal_values(stream_key, dims, width, reach, shards=(), kind=jnp.bfloat16):
    result = width * jax.random.normal(stream_key, dims, jnp.float32)
    if shards:
        result = result * level_of(stream_key, dims, shards, -0.22, 0.18)
    return jnp.clip(result, -reach, reach).astype(kind)


def setup_inputs(seed: int = 0) -> dict:
    key_list = jax.random.split(jax.random.key(seed), 9)
    return {
        "states": normal_values(key_list[0], (STATES, NODES), 1.0, 6.0, ((1, 128),), jnp.float32),
        "block_part": draw_block_part(jax.random.fold_in(key_list[8], 71), 0),
        "tile_perm": jax.vmap(lambda own: jax.random.permutation(own, NODE_BLK))(jax.random.split(key_list[2], BLOCKS)).reshape((BLOCKS, NODE_BLK)).astype(jnp.int32),
        "half_volt": normal_values(key_list[3], (GATES,), 1.0, 4.0, (), jnp.float32),
        "steepness": jnp.clip(jnp.exp(jax.random.uniform(key_list[4], (GATES,), jnp.float32, math.log(0.5), math.log(4.0))), 0.5, 4.0),
        "gate_rate": jnp.clip(jnp.exp(jax.random.uniform(key_list[5], (GATES,), jnp.float32, math.log(0.1), math.log(1.0))), 0.1, 1.0),
        "conductance": jnp.clip(jnp.exp(jax.random.uniform(key_list[6], (GATES,), jnp.float32, math.log(0.005), math.log(0.08))), 0.005, 0.08),
        "reversal": normal_values(key_list[7], (GATES,), 1.5, 6.0, (), jnp.float32),
    }


time_step = 0.25


def advance(state_rows, half_volt, steepness, gate_rate, conductance, reversal):
    voltage = state_rows[0:1]
    gate_vals = state_rows[1:]
    for substep in range(SUBSTEPS):
        steady = jax.nn.sigmoid((voltage - half_volt[:, None]) * steepness[:, None])
        damping = jnp.exp(-gate_rate[:, None] * (1.0 + jax.nn.sigmoid(voltage)))
        gate_vals = steady + (gate_vals - steady) * damping
        current = jnp.sum(conductance[:, None] * gate_vals * (voltage - reversal[:, None]), axis=0, keepdims=True)
        voltage = voltage - time_step * current
    return jnp.concatenate([voltage, gate_vals], axis=0)


def reference(states, block_part, tile_perm, half_volt, steepness, gate_rate, conductance, reversal):
    devices = BLOCKS // BLK_DEV
    span = BLK_DEV * NODE_BLK

    def one_part(index, acc):
        start = (index * span).astype(jnp.int32)
        piece = lax.dynamic_slice_in_dim(states, start, span, 1)
        done = advance(piece, half_volt, steepness, gate_rate, conductance, reversal)
        return lax.dynamic_update_slice_in_dim(acc, done, start, 1)

    advanced = lax.fori_loop(0, devices, one_part, jnp.zeros_like(states))
    ordering = jnp.argsort(block_part, stable=True).astype(jnp.int32)
    local_index = jnp.zeros((BLOCKS,), jnp.int32).at[ordering].set(jnp.arange(BLOCKS, dtype=jnp.int32))
    columns = (local_index[:, None] * NODE_BLK + tile_perm).reshape(-1).astype(jnp.int32)
    return jnp.take(advanced, columns, axis=1)
```

```python
import functools

import jax
import jax.numpy as jnp
from jax import lax
from jax.experimental import pallas as pl
from jax.experimental.pallas import tpu as pltpu
from jax.sharding import PartitionSpec as P

AXES = ("group", "peer")
DEVICES = 128
BLOCKS = 256
LANES = 128
ROWS = 41
CAP = 4
TIME_STEP = 0.25


def advance(block, half_volt, steepness, gate_rate, conductance, reversal):
    voltage = block[0:1, :]
    steady = jax.nn.sigmoid((voltage - half_volt) * steepness)
    damping = jnp.exp(-gate_rate * (1.0 + jax.nn.sigmoid(voltage)))
    gates = steady + (block - steady) * damping
    current = jnp.sum(conductance * gates * (voltage - reversal), axis=0, keepdims=True)
    row = lax.broadcasted_iota(jnp.int32, block.shape, 0)
    return jnp.where(row == 0, voltage - TIME_STEP * current, gates)


def pack_kernel(per_step, starts_ref, states_ref, hv, st, gr, co, re, out_ref):
    step = pl.program_id(0)
    params = [r[...] for r in (hv, st, gr, co, re)]
    for j in range(per_step):
        first = starts_ref[step * per_step + j]
        for k in range(CAP):
            at = jnp.minimum(first + k, BLOCKS - 1)
            block = states_ref[:, pl.ds(pl.multiple_of(at * LANES, LANES), LANES)]
            out_ref[j, k * ROWS:(k + 1) * ROWS, :] = advance(block, *params)


def place_kernel(per_step, slots_ref, arrived_ref, perm_ref, out_ref):
    step = pl.program_id(0)
    for j in range(per_step):
        slot = slots_ref[step * per_step + j]
        part, rank = slot // CAP, slot % CAP
        block = arrived_ref[part, pl.ds(rank * ROWS, ROWS), :]
        index = jnp.broadcast_to(perm_ref[j:j + 1, :], (ROWS, LANES))
        out_ref[:, j * LANES:(j + 1) * LANES] = jnp.take_along_axis(block, index, axis=1)


def row_params(values, dummy):
    padded = jnp.concatenate([jnp.full((1,), dummy, values.dtype), values])
    return jnp.broadcast_to(padded[:, None], (ROWS, LANES))


def on_device(states, block_part, tile_perm, half_volt, steepness, gate_rate, conductance, reversal):
    me = lax.axis_index(AXES)
    parts = jnp.arange(DEVICES, dtype=jnp.int32)
    onehot = (block_part[:, None] == parts[None, :]).astype(jnp.float32)
    order = jnp.arange(BLOCKS, dtype=jnp.int32)
    lower = (order[:, None] > order[None, :]).astype(jnp.float32)
    before = lax.dot(lower, onehot)
    rank = jnp.sum(onehot * before, axis=1).astype(jnp.int32)
    slots = block_part * CAP + rank
    counts = jnp.sum(onehot, axis=0).astype(jnp.int32)
    every = lax.all_gather(counts, AXES)
    mine = jnp.sum(jnp.where(parts[None, :] == me, every, 0), axis=1).astype(jnp.float32)
    starts = lax.dot((parts[:, None] > parts[None, :]).astype(jnp.float32), mine).astype(jnp.int32)

    params = [
        row_params(half_volt, 0.0),
        row_params(steepness, 1.0),
        row_params(gate_rate, 1.0),
        row_params(conductance, 0.0),
        row_params(reversal, 0.0),
    ]
    whole = pl.BlockSpec(memory_space=pltpu.VMEM)
    smem = pl.BlockSpec(memory_space=pltpu.SMEM)
    per = 8
    served = pl.pallas_call(
        functools.partial(pack_kernel, per),
        grid=(DEVICES // per,),
        out_shape=jax.ShapeDtypeStruct((DEVICES, CAP * ROWS, LANES), jnp.float32),
        in_specs=[smem, whole] + [whole] * 5,
        out_specs=pl.BlockSpec((per, CAP * ROWS, LANES), lambda i: (i, 0, 0)),
        compiler_params=pltpu.CompilerParams(vmem_limit_bytes=32 * 1024 * 1024),
    )(starts, states, *params)
    arrived = lax.all_to_all(served, AXES, split_axis=0, concat_axis=0, tiled=True)
    per = 16
    return pl.pallas_call(
        functools.partial(place_kernel, per),
        grid=(BLOCKS // per,),
        out_shape=jax.ShapeDtypeStruct((ROWS, BLOCKS * LANES), jnp.float32),
        in_specs=[smem, whole, pl.BlockSpec((per, LANES), lambda i: (i, 0))],
        out_specs=pl.BlockSpec((ROWS, per * LANES), lambda i: (0, i)),
        compiler_params=pltpu.CompilerParams(vmem_limit_bytes=32 * 1024 * 1024),
    )(slots, arrived, tile_perm)


def solution(mesh):
    split = P(None, AXES)
    placed = (split, P(AXES), P(AXES, None), P(), P(), P(), P(), P())
    return jax.shard_map(on_device, mesh=mesh, in_specs=placed, out_specs=split, check_vma=False)
```

```python
import functools

import jax
import jax.numpy as jnp
from jax import lax
from jax.experimental import pallas as pl
from jax.experimental.pallas import tpu as pltpu
from jax.sharding import PartitionSpec as P

AXES = ("group", "peer")
DEVICES = 128
BLOCKS = 256
LANES = 128
ROWS = 41
SLOTS = 4
TIME_STEP = 0.25
PIECE = 7
LIMIT = 176
SIZES = (4, 2, 4, 4)
STRIDES = (32, 16, 4, 1)
CORE = 1
ORDERS = ((3, 0, 2), (0, 2, 3), (2, 3, 0))
MESH = pl.DeviceIdType.MESH


def digits_of(device):
    return tuple(lax.rem(lax.div(device, st), sz) for st, sz in zip(STRIDES, SIZES))


def take_digits(number, dims):
    out = {}
    for d in reversed(dims):
        out[d] = lax.rem(number, SIZES[d])
        number = lax.div(number, SIZES[d])
    return out, number


def cells(stage, order, own, r):
    if stage == 3:
        fixed_s, free_p, list_dim, held_by = tuple(order), (0, 1, 2, 3), CORE, order[2]
    else:
        fixed_s = tuple(order[:stage])
        free_p = tuple(sorted(fixed_s + (CORE,)))
        list_dim = order[stage]
        held_by = CORE if stage == 0 else order[stage - 1]
    free_s = tuple(d for d in range(4) if d not in fixed_s and d != list_dim)
    s, rest = take_digits(r, free_s)
    p, rest = take_digits(rest, free_p)
    s[list_dim] = rest
    slab = sum((s[d] if d in s else own[d]) * STRIDES[d] for d in range(4))
    part = sum((p[d] if d in p else own[d]) * STRIDES[d] for d in range(4))
    return slab, part, p[held_by]


def index_lists(stage, order, own, counts, cap):
    lists = 2 if stage == 3 else 4
    size = 256 // lists
    col = lax.broadcasted_iota(jnp.int32, (256, 1), 0)
    row = lax.broadcasted_iota(jnp.int32, (1, 256), 1)
    slab, part, held = cells(stage, order, own, col)
    slab_r, part_r, held_r = cells(stage, order, own, row)
    device = lax.broadcasted_iota(jnp.int32, (1, DEVICES), 1)
    pick = (part == device).astype(jnp.float32)
    by_part = lax.dot_general(pick, counts, (((1,), (1,)), ((), ())))
    n = jnp.sum(jnp.where(slab == device, by_part, 0.0), axis=1, keepdims=True)
    earlier = (held_r == held) & (part_r * DEVICES + slab_r < part * DEVICES + slab)
    base = lax.dot(earlier.astype(jnp.float32), n).astype(jnp.int32)
    base = base + held * (BLOCKS if stage == 0 else cap)
    same = lax.div(row, size) == lax.div(col, size)
    place = lax.dot((same & (row < col)).astype(jnp.float32), n).astype(jnp.int32)
    n = n.astype(jnp.int32)
    out = []
    j = lax.broadcasted_iota(jnp.int32, (1, 256), 1)
    for k in range(lists):
        part_of = slice(k * size, (k + 1) * size)
        lo, shift, width = place[part_of], (base - place)[part_of], n[part_of]
        inside = (j >= lo) & (j < lo + width)
        out.append(j + jnp.sum(jnp.where(inside, shift, 0), axis=0, keepdims=True))
    return jnp.concatenate(out, axis=0)


def longest_list(counts):
    grid = counts.reshape(SIZES + SIZES)
    longest = []
    for order in ORDERS:
        for stage in range(3):
            done, to = order[:stage], order[:stage + 1]
            keep = set(d for d in (0, 2, 3) if d not in done)
            axes = tuple(d for d in range(4) if d not in to) + tuple(4 + d for d in range(4) if d not in keep)
            longest.append(jnp.max(jnp.sum(grid, axis=axes)))
    return functools.reduce(jnp.maximum, longest)


def advance(block, half_volt, steepness, gate_rate, conductance, reversal):
    voltage = block[0:1, :]
    steady = jax.nn.sigmoid((voltage - half_volt) * steepness)
    damping = jnp.exp(-gate_rate * (1.0 + jax.nn.sigmoid(voltage)))
    gates = steady + (block - steady) * damping
    current = jnp.sum(conductance * gates * (voltage - reversal), axis=0, keepdims=True)
    row = lax.broadcasted_iota(jnp.int32, block.shape, 0)
    return jnp.where(row == 0, voltage - TIME_STEP * current, gates)


def move_kernel(cap, lists_ref, states_ref, hv, st, gr, co, re, out_ref, *scratch):
    adv, recv, stage, send = scratch[:3], (scratch[3:6], scratch[6:9], scratch[9:12]), scratch[12], scratch[13]
    swap_send, swap_recv, send_sem, recv_sem, last_send, last_recv = scratch[14:]
    me = lax.axis_index("group") * 16 + lax.axis_index("peer")
    own = digits_of(me)
    core = own[CORE]

    def at(coords):
        return (coords[0] * 2 + coords[CORE], coords[2] * 4 + coords[3])

    partner = at((own[0], 1 - core, own[2], own[3]))
    params = [r[...] for r in (hv, st, gr, co, re)]
    half = 3 * PIECE
    mine_at = core * (BLOCKS * PIECE)

    def update(i, carry):
        for u in range(8):
            b = i * 8 + u
            new = advance(states_ref[:, pl.ds(pl.multiple_of(b * LANES, LANES), LANES)], *params)
            low = new[0:half]
            high = jnp.concatenate([new[half:ROWS], new[ROWS - 1:ROWS]], axis=0)
            keep = jnp.where(core == 0, low, high)
            give = jnp.where(core == 0, high, low)
            for t in range(3):
                adv[t][pl.ds(mine_at + b * PIECE, PIECE), :] = keep[t * PIECE:(t + 1) * PIECE]
                stage[t, pl.ds(b * PIECE, PIECE), :] = give[t * PIECE:(t + 1) * PIECE]
        return carry

    lax.fori_loop(0, BLOCKS // 8, update, 0)

    def swap(t):
        return pltpu.make_async_remote_copy(
            src_ref=stage.at[t],
            dst_ref=adv[t].at[pl.ds(pl.multiple_of(mine_at, 8), BLOCKS * PIECE)],
            send_sem=swap_send.at[t], recv_sem=swap_recv.at[t], device_id=partner, device_id_type=MESH)

    for t in range(3):
        swap(t).start()

    def hop(t, ph, delta):
        dim = ORDERS[t][ph]
        to = lax.rem(own[dim] + delta, 4)
        coords = tuple(to if d == dim else own[d] for d in range(4))
        return pltpu.make_async_remote_copy(
            src_ref=send.at[t, delta - 1],
            dst_ref=recv[ph][t].at[pl.ds(pl.multiple_of(own[dim] * (cap * PIECE), 8), cap * PIECE)],
            send_sem=send_sem.at[ph, t, delta - 1], recv_sem=recv_sem.at[ph, t, delta - 1],
            device_id=at(coords), device_id_type=MESH)

    def gather(source, target, start, row, count):
        def body(i, carry):
            for u in range(8):
                j = i * 8 + u
                target[pl.ds(start + j * PIECE, PIECE), :] = source[pl.ds(lists_ref[row, j] * PIECE, PIECE), :]
            return carry

        lax.fori_loop(0, count // 8, body, 0)

    for ph in range(3):
        for t in range(3):
            dim = ORDERS[t][ph]
            if ph == 0:
                swap(t).wait()
                source = adv[t]
            else:
                for delta in (2, 1, 3):
                    hop(t, ph - 1, delta).wait()
                source = recv[ph - 1][t]
            for delta in (2, 1, 3, 0):
                to = lax.rem(own[dim] + delta, 4)
                row = (ph * 3 + t) * 4 + to
                if delta:
                    gather(source, send.at[t, delta - 1], 0, row, cap)
                    hop(t, ph, delta).start()
                else:
                    gather(source, recv[ph][t], own[dim] * (cap * PIECE), row, cap)

    def last(t):
        return pltpu.make_async_remote_copy(
            src_ref=stage.at[t], dst_ref=out_ref.at[core, t],
            send_sem=last_send.at[t], recv_sem=last_recv.at[t], device_id=partner, device_id_type=MESH)

    for t in range(3):
        for delta in (2, 1, 3):
            hop(t, 2, delta).wait()
        gather(recv[2][t], stage.at[t], 0, 36 + t * 2 + 1 - core, BLOCKS)
        last(t).start()
    for t in range(3):
        gather(recv[2][t], out_ref.at[core, t], 0, 36 + t * 2 + core, BLOCKS)
    for t in range(3):
        last(t).wait()


def settle_kernel(per_step, where_ref, parts_ref, perm_ref, out_ref):
    step = pl.program_id(0)
    for j in range(per_step):
        at = where_ref[step * per_step + j] * PIECE
        rows = [parts_ref[h, t, pl.ds(at, PIECE), :] for h in range(2) for t in range(3)]
        block = jnp.concatenate(rows, axis=0)[0:ROWS]
        index = jnp.broadcast_to(perm_ref[j:j + 1, :], (ROWS, LANES))
        out_ref[:, j * LANES:(j + 1) * LANES] = jnp.take_along_axis(block, index, axis=1)


def pack_kernel(per_step, starts_ref, states_ref, hv, st, gr, co, re, out_ref):
    step = pl.program_id(0)
    params = [r[...] for r in (hv, st, gr, co, re)]
    for j in range(per_step):
        first = starts_ref[step * per_step + j]
        for k in range(SLOTS):
            at = jnp.minimum(first + k, BLOCKS - 1)
            block = states_ref[:, pl.ds(pl.multiple_of(at * LANES, LANES), LANES)]
            out_ref[j, k * ROWS:(k + 1) * ROWS, :] = advance(block, *params)


def place_kernel(per_step, slots_ref, arrived_ref, perm_ref, out_ref):
    step = pl.program_id(0)
    for j in range(per_step):
        slot = slots_ref[step * per_step + j]
        part, rank = slot // SLOTS, slot % SLOTS
        block = arrived_ref[part, pl.ds(rank * ROWS, ROWS), :]
        index = jnp.broadcast_to(perm_ref[j:j + 1, :], (ROWS, LANES))
        out_ref[:, j * LANES:(j + 1) * LANES] = jnp.take_along_axis(block, index, axis=1)


def row_params(values, dummy):
    padded = jnp.concatenate([jnp.full((1,), dummy, values.dtype), values])
    return jnp.broadcast_to(padded[:, None], (ROWS, LANES))


WHOLE = pl.BlockSpec(memory_space=pltpu.VMEM)
SCALARS = pl.BlockSpec(memory_space=pltpu.SMEM)


def direct_route(counts, states, params, block_part, rank, tile_perm):
    me = lax.axis_index(AXES)
    parts = jnp.arange(DEVICES, dtype=jnp.int32)
    mine = jnp.sum(jnp.where(parts[None, :] == me, counts, 0.0), axis=1)
    starts = lax.dot((parts[:, None] > parts[None, :]).astype(jnp.float32), mine).astype(jnp.int32)
    per = 8
    served = pl.pallas_call(
        functools.partial(pack_kernel, per),
        grid=(DEVICES // per,),
        out_shape=jax.ShapeDtypeStruct((DEVICES, SLOTS * ROWS, LANES), jnp.float32),
        in_specs=[SCALARS, WHOLE] + [WHOLE] * 5,
        out_specs=pl.BlockSpec((per, SLOTS * ROWS, LANES), lambda i: (i, 0, 0)),
        compiler_params=pltpu.CompilerParams(vmem_limit_bytes=32 * 1024 * 1024),
    )(starts, states, *params)
    arrived = lax.all_to_all(served, AXES, split_axis=0, concat_axis=0, tiled=True)
    per = 16
    return pl.pallas_call(
        functools.partial(place_kernel, per),
        grid=(BLOCKS // per,),
        out_shape=jax.ShapeDtypeStruct((ROWS, BLOCKS * LANES), jnp.float32),
        in_specs=[SCALARS, WHOLE, pl.BlockSpec((per, LANES), lambda i: (i, 0))],
        out_specs=pl.BlockSpec((ROWS, per * LANES), lambda i: (0, i)),
        compiler_params=pltpu.CompilerParams(vmem_limit_bytes=32 * 1024 * 1024),
    )(block_part * SLOTS + rank, arrived, tile_perm)


def staged_route(cap, counts, states, params, block_part, rank, tile_perm):
    me = lax.axis_index("group") * 16 + lax.axis_index("peer")
    own = digits_of(me)
    lists = [index_lists(ph, ORDERS[t], own, counts, cap) for ph in range(3) for t in range(3)]
    lists += [index_lists(3, ORDERS[t], own, counts, cap) for t in range(3)]
    lists = jnp.concatenate(lists, axis=0)
    dma = pltpu.SemaphoreType.DMA
    parts = pl.pallas_call(
        functools.partial(move_kernel, cap),
        out_shape=jax.ShapeDtypeStruct((2, 3, BLOCKS * PIECE, LANES), jnp.float32),
        in_specs=[SCALARS, WHOLE] + [WHOLE] * 5,
        out_specs=WHOLE,
        scratch_shapes=[
            *[pltpu.VMEM((2 * BLOCKS * PIECE, LANES), jnp.float32)] * 3,
            *[pltpu.VMEM((4 * cap * PIECE, LANES), jnp.float32)] * 9,
            pltpu.VMEM((3, BLOCKS * PIECE, LANES), jnp.float32),
            pltpu.VMEM((3, 3, cap * PIECE, LANES), jnp.float32),
            dma((3,)), dma((3,)), dma((3, 3, 3)), dma((3, 3, 3)), dma((3,)), dma((3,)),
        ],
        compiler_params=pltpu.CompilerParams(has_side_effects=True, vmem_limit_bytes=60 * 1024 * 1024),
    )(lists, states, *params)
    number = jnp.arange(DEVICES, dtype=jnp.int32)
    ours = jnp.sum(jnp.where(number[:, None] == me, counts, 0.0), axis=0)
    ahead = lax.dot((number[:, None] > number[None, :]).astype(jnp.float32), ours)
    onehot = block_part[:, None] == number[None, :]
    where = jnp.sum(jnp.where(onehot, ahead[None, :], 0.0), axis=1).astype(jnp.int32) + rank
    per = 16
    return pl.pallas_call(
        functools.partial(settle_kernel, per),
        grid=(BLOCKS // per,),
        out_shape=jax.ShapeDtypeStruct((ROWS, BLOCKS * LANES), jnp.float32),
        in_specs=[SCALARS, WHOLE, pl.BlockSpec((per, LANES), lambda i: (i, 0))],
        out_specs=pl.BlockSpec((ROWS, per * LANES), lambda i: (0, i)),
        compiler_params=pltpu.CompilerParams(vmem_limit_bytes=32 * 1024 * 1024),
    )(where, parts, tile_perm)


def on_device(states, block_part, tile_perm, half_volt, steepness, gate_rate, conductance, reversal):
    parts = jnp.arange(DEVICES, dtype=jnp.int32)
    onehot = (block_part[:, None] == parts[None, :]).astype(jnp.float32)
    order = jnp.arange(BLOCKS, dtype=jnp.int32)
    before = lax.dot((order[:, None] > order[None, :]).astype(jnp.float32), onehot)
    rank = jnp.sum(onehot * before, axis=1).astype(jnp.int32)
    counts = jnp.sum(onehot, axis=0)
    counts = lax.all_gather(counts, "peer")
    counts = lax.all_gather(counts, "group").reshape(DEVICES, DEVICES)
    params = [
        row_params(half_volt, 0.0),
        row_params(steepness, 1.0),
        row_params(gate_rate, 1.0),
        row_params(conductance, 0.0),
        row_params(reversal, 0.0),
    ]
    fits = longest_list(counts) <= LIMIT
    args = (counts, states, params, block_part, rank, tile_perm)
    return lax.cond(fits, functools.partial(staged_route, LIMIT), direct_route, *args)


def solution(mesh):
    split = P(None, AXES)
    placed = (split, P(AXES), P(AXES, None), P(), P(), P(), P(), P())
    return jax.shard_map(on_device, mesh=mesh, in_specs=placed, out_specs=split, check_vma=False)
```

```python
import functools

import jax
import jax.numpy as jnp
from jax import lax
from jax.experimental import pallas as pl
from jax.experimental.pallas import tpu as pltpu
from jax.sharding import PartitionSpec as P

AXES = ("group", "peer")
DEVICES = 128
BLOCKS = 256
LANES = 128
ROWS = 41
SLOTS = 4
TIME_STEP = 0.25
PIECE = 7
LIMIT = 176
SIZES = (4, 2, 4, 4)
STRIDES = (32, 16, 4, 1)
CORE = 1
ORDERS = ((3, 0, 2), (0, 2, 3), (2, 3, 0))
MESH = pl.DeviceIdType.MESH


def digits_of(device):
    return tuple(lax.rem(lax.div(device, st), n) for st, n in zip(STRIDES, SIZES))


def take_digits(number, dims):
    out = {}
    for d in reversed(dims):
        out[d] = number & (SIZES[d] - 1)
        number = number >> (SIZES[d].bit_length() - 1)
    return out, number


def cells(stage, order, own, r):
    if stage == 3:
        fixed_s, free_p, list_dim, held_by = tuple(order), (0, 1, 2, 3), CORE, order[2]
    else:
        fixed_s = tuple(order[:stage])
        free_p = tuple(sorted(fixed_s + (CORE,)))
        list_dim = order[stage]
        held_by = CORE if stage == 0 else order[stage - 1]
    free_s = tuple(d for d in range(4) if d not in fixed_s and d != list_dim)
    s, rest = take_digits(r, free_s)
    p, rest = take_digits(rest, free_p)
    s[list_dim] = rest
    slab = sum((s[d] if d in s else own[d]) * STRIDES[d] for d in range(4))
    part = sum((p[d] if d in p else own[d]) * STRIDES[d] for d in range(4))
    return slab, part, p[held_by]


def index_lists(stage, order, own, counts, cap):
    lists = 2 if stage == 3 else 4
    size = 256 // lists
    col = lax.broadcasted_iota(jnp.int32, (256, 1), 0)
    row = lax.broadcasted_iota(jnp.int32, (1, 256), 1)
    slab, part, held = cells(stage, order, own, col)
    slab_r, part_r, held_r = cells(stage, order, own, row)
    device = lax.broadcasted_iota(jnp.int32, (1, DEVICES), 1)
    pick = (part == device).astype(jnp.float32)
    by_part = lax.dot_general(pick, counts, (((1,), (1,)), ((), ())), preferred_element_type=jnp.float32)
    n = jnp.sum(jnp.where(slab == device, by_part, 0.0), axis=1, keepdims=True)
    wide = jnp.broadcast_to(n, (256, LANES))
    earlier = (held_r == held) & (part_r * DEVICES + slab_r < part * DEVICES + slab)
    base = jnp.dot(earlier.astype(jnp.float32), wide, preferred_element_type=jnp.float32)[:, 0:1].astype(jnp.int32)
    base = base + held * (BLOCKS if stage == 0 else cap)
    shift = size.bit_length() - 1
    ahead = ((row >> shift) == (col >> shift)) & (row < col)
    place = jnp.dot(ahead.astype(jnp.float32), wide, preferred_element_type=jnp.float32)[:, 0:1].astype(jnp.int32)
    end = place + n.astype(jnp.int32)
    gap = base - place
    limit = 2 * BLOCKS - 1 if stage == 0 else 4 * cap - 1
    out = []
    for k in range(lists):
        one = slice(k * size, (k + 1) * size)
        inside = (row >= place[one]) & (row < end[one])
        found = row + jnp.sum(jnp.where(inside, gap[one], 0), axis=0, keepdims=True)
        out.append(jnp.clip(found, 0, limit))
    return out


def same_key(dims):
    i = lax.broadcasted_iota(jnp.int32, (DEVICES, DEVICES), 0)
    j = lax.broadcasted_iota(jnp.int32, (DEVICES, DEVICES), 1)
    mask = sum((SIZES[d] - 1) * STRIDES[d] for d in dims)
    return ((i & mask) == (j & mask)).astype(jnp.float32)


def longest_list(counts):
    longest = None
    for order in ORDERS:
        for stage in range(3):
            to, left = order[:stage + 1], order[stage:]
            sums = jnp.dot(same_key(to), counts, preferred_element_type=jnp.float32)
            sums = jnp.dot(sums, same_key(left), preferred_element_type=jnp.float32)
            longest = sums if longest is None else jnp.maximum(longest, sums)
    return jnp.max(longest, axis=0, keepdims=True)


def advance(block, half_volt, steepness, gate_rate, conductance, reversal):
    voltage = block[0:1, :]
    steady = jax.nn.sigmoid((voltage - half_volt) * steepness)
    damping = jnp.exp(-gate_rate * (1.0 + jax.nn.sigmoid(voltage)))
    gates = steady + (block - steady) * damping
    current = jnp.sum(conductance * gates * (voltage - reversal), axis=0, keepdims=True)
    row = lax.broadcasted_iota(jnp.int32, block.shape, 0)
    return jnp.where(row == 0, voltage - TIME_STEP * current, gates)


def column(values):
    lane = lax.broadcasted_iota(jnp.int32, (ROWS, ROWS - 1), 1)
    row = lax.broadcasted_iota(jnp.int32, (ROWS, ROWS - 1), 0)
    picked = jnp.sum(jnp.where(lane == row - 1, values, 0.0), axis=1, keepdims=True)
    return jnp.broadcast_to(picked, (ROWS, LANES))


CHUNKS = 4
CHUNK = BLOCKS // CHUNKS


def move_kernel(cap, part_ref, states_ref, hv, st, gr, co, re, out_ref, where_ref, longest_ref, counts_ref, *scratch):
    adv, recv, stage, send = scratch[:3], (scratch[3:6], scratch[6:9], scratch[9:12]), scratch[12], scratch[13]
    states, tables, lists = scratch[14], scratch[15], scratch[16:28]
    (load_sem, table_sem, count_send, count_recv, swap_send, swap_recv, send_sem, recv_sem,
     last_send, last_recv) = scratch[28:]
    me = lax.axis_index("group") * 16 + lax.axis_index("peer")
    own = digits_of(me)
    core = own[CORE]

    def at(coords):
        return (coords[0] * 2 + coords[CORE], coords[2] * 4 + coords[3])

    def along(dim, delta):
        to = lax.rem(own[dim] + delta, SIZES[dim])
        return at(tuple(to if d == dim else own[d] for d in range(4)))

    def load(k):
        columns = pl.ds(k * CHUNK * LANES, CHUNK * LANES)
        return pltpu.make_async_copy(states_ref.at[:, columns], states.at[:, columns], load_sem.at[k])

    for k in range(CHUNKS):
        load(k).start()
    barrier = pltpu.get_barrier_semaphore()
    neighbours = [(d, delta) for d in range(4) for delta in range(1, SIZES[d])]
    for d, delta in neighbours:
        pl.semaphore_signal(barrier, inc=1, device_id=along(d, delta), device_id_type=MESH)

    parts = part_ref[...]
    onehot = (lax.broadcasted_iota(jnp.int32, (DEVICES, BLOCKS), 0) == parts).astype(jnp.float32)
    ones = jnp.ones((8, BLOCKS), jnp.float32)
    mine = lax.dot_general(ones, onehot, (((1,), (1,)), ((), ())), preferred_element_type=jnp.float32)[0:1]
    counts_ref[me] = mine
    params = [column(r[...]) for r in (hv, st, gr, co, re)]

    pl.semaphore_wait(barrier, len(neighbours))

    spread = (3, 2, 1, 0)

    def tell(k, delta):
        held = STRIDES[spread[k]]
        rows = pl.ds(lax.div(me, held) * held, held)
        return pltpu.make_async_remote_copy(
            src_ref=counts_ref.at[rows], dst_ref=counts_ref.at[rows],
            send_sem=count_send.at[k, delta - 1], recv_sem=count_recv.at[k, delta - 1],
            device_id=along(spread[k], delta), device_id_type=MESH)

    half = 3 * PIECE
    mine_at = core * (BLOCKS * PIECE)

    def update(i, carry):
        for u in range(8):
            b = i * 8 + u
            new = advance(states[:, pl.ds(pl.multiple_of(b * LANES, LANES), LANES)], *params)
            low = new[0:half]
            high = jnp.concatenate([new[half:ROWS], new[ROWS - 1:ROWS]], axis=0)
            keep = jnp.where(core == 0, low, high)
            give = jnp.where(core == 0, high, low)
            for t in range(3):
                adv[t][pl.ds(mine_at + b * PIECE, PIECE), :] = keep[t * PIECE:(t + 1) * PIECE]
                stage[t, pl.ds(b * PIECE, PIECE), :] = give[t * PIECE:(t + 1) * PIECE]
        return carry

    def swap(t, k):
        rows = CHUNK * PIECE
        return pltpu.make_async_remote_copy(
            src_ref=stage.at[t, pl.ds(k * rows, rows)],
            dst_ref=adv[t].at[pl.ds(pl.multiple_of(mine_at + k * rows, 8), rows)],
            send_sem=swap_send.at[t, k], recv_sem=swap_recv.at[t, k],
            device_id=along(CORE, 1), device_id_type=MESH)

    for k in range(CHUNKS):
        for delta in range(1, SIZES[spread[k]]):
            tell(k, delta).start()
        load(k).wait()
        lax.fori_loop(k * CHUNK // 8, (k + 1) * CHUNK // 8, update, 0)
        for t in range(3):
            swap(t, k).start()
        for delta in range(1, SIZES[spread[k]]):
            tell(k, delta).wait()

    counts = counts_ref[...].reshape(DEVICES, DEVICES)

    def table(ph, t):
        return pltpu.make_async_copy(tables.at[ph * 3 + t], lists[ph * 3 + t], table_sem.at[ph * 3 + t])

    def make_table(ph, t):
        found = index_lists(ph, ORDERS[t], own, counts, cap)
        for k, one in enumerate(found):
            tables[ph * 3 + t, k:k + 1, :] = one

    for t in range(3):
        make_table(0, t)
    for t in range(3):
        table(0, t).start()

    def hop(t, ph, delta):
        dim = ORDERS[t][ph]
        return pltpu.make_async_remote_copy(
            src_ref=send.at[t, delta - 1],
            dst_ref=recv[ph][t].at[pl.ds(pl.multiple_of(own[dim] * (cap * PIECE), 8), cap * PIECE)],
            send_sem=send_sem.at[ph, t, delta - 1], recv_sem=recv_sem.at[ph, t, delta - 1],
            device_id=along(dim, delta), device_id_type=MESH)

    def gather(source, target, start, which, row, count):
        def body(i, carry):
            for u in range(8):
                j = i * 8 + u
                target[pl.ds(start + j * PIECE, PIECE), :] = source[pl.ds(which[row, j] * PIECE, PIECE), :]
            return carry

        lax.fori_loop(0, count // 8, body, 0)

    for ph in range(3):
        for t in range(3):
            dim = ORDERS[t][ph]
            table(ph, t).wait()
            if ph == 0:
                for k in range(CHUNKS):
                    swap(t, k).wait()
                source = adv[t]
            else:
                for delta in (2, 1, 3):
                    hop(t, ph - 1, delta).wait()
                source = recv[ph - 1][t]
            for delta in (2, 1, 3, 0):
                to = lax.rem(own[dim] + delta, 4)
                if delta:
                    gather(source, send.at[t, delta - 1], 0, lists[ph * 3 + t], to, cap)
                    hop(t, ph, delta).start()
                else:
                    gather(source, recv[ph][t], own[dim] * (cap * PIECE), lists[ph * 3 + t], to, cap)
        for t in range(3):
            make_table(ph + 1, t)
        for t in range(3):
            table(ph + 1, t).start()
        if ph == 0:
            longest_ref[0, 0] = jnp.max(longest_list(counts)).astype(jnp.int32)
            r = lax.broadcasted_iota(jnp.int32, (BLOCKS, BLOCKS), 0)
            c = lax.broadcasted_iota(jnp.int32, (BLOCKS, BLOCKS), 1)
            before = jnp.dot(onehot, (r < c).astype(jnp.float32), preferred_element_type=jnp.float32)
            d = lax.broadcasted_iota(jnp.int32, (DEVICES, DEVICES), 0)
            e = lax.broadcasted_iota(jnp.int32, (DEVICES, DEVICES), 1)
            ahead = jnp.sum(jnp.where(e < d, mine, 0.0), axis=1, keepdims=True)
            where_ref[...] = jnp.sum(onehot * (before + ahead), axis=0, keepdims=True).astype(jnp.int32)

    def last(t):
        return pltpu.make_async_remote_copy(
            src_ref=stage.at[t], dst_ref=out_ref.at[core, t],
            send_sem=last_send.at[t], recv_sem=last_recv.at[t],
            device_id=along(CORE, 1), device_id_type=MESH)

    for t in range(3):
        table(3, t).wait()
        for delta in (2, 1, 3):
            hop(t, 2, delta).wait()
        gather(recv[2][t], stage.at[t], 0, lists[9 + t], 1 - core, BLOCKS)
        last(t).start()
    for t in range(3):
        gather(recv[2][t], out_ref.at[core, t], 0, lists[9 + t], core, BLOCKS)
    for t in range(3):
        last(t).wait()


def settle_kernel(per_step, where_ref, parts_ref, perm_ref, out_ref):
    step = pl.program_id(0)
    for j in range(per_step):
        at = where_ref[step * per_step + j] * PIECE
        rows = [parts_ref[h, t, pl.ds(at, PIECE), :] for h in range(2) for t in range(3)]
        block = jnp.concatenate(rows, axis=0)[0:ROWS]
        index = jnp.broadcast_to(perm_ref[j:j + 1, :], (ROWS, LANES))
        out_ref[:, j * LANES:(j + 1) * LANES] = jnp.take_along_axis(block, index, axis=1)


def pack_kernel(per_step, starts_ref, states_ref, hv, st, gr, co, re, out_ref):
    step = pl.program_id(0)
    params = [r[...] for r in (hv, st, gr, co, re)]
    for j in range(per_step):
        first = starts_ref[step * per_step + j]
        for k in range(SLOTS):
            at = jnp.minimum(first + k, BLOCKS - 1)
            block = states_ref[:, pl.ds(pl.multiple_of(at * LANES, LANES), LANES)]
            out_ref[j, k * ROWS:(k + 1) * ROWS, :] = advance(block, *params)


def place_kernel(per_step, slots_ref, arrived_ref, perm_ref, out_ref):
    step = pl.program_id(0)
    for j in range(per_step):
        slot = slots_ref[step * per_step + j]
        part, rank = slot // SLOTS, slot % SLOTS
        block = arrived_ref[part, pl.ds(rank * ROWS, ROWS), :]
        index = jnp.broadcast_to(perm_ref[j:j + 1, :], (ROWS, LANES))
        out_ref[:, j * LANES:(j + 1) * LANES] = jnp.take_along_axis(block, index, axis=1)


def row_params(values, dummy):
    padded = jnp.concatenate([jnp.full((1,), dummy, values.dtype), values])
    return jnp.broadcast_to(padded[:, None], (ROWS, LANES))


WHOLE = pl.BlockSpec(memory_space=pltpu.VMEM)
SCALARS = pl.BlockSpec(memory_space=pltpu.SMEM)


def direct_route(parts, where, counts, states, block_part, tile_perm, *values):
    me = lax.axis_index(AXES)
    number = jnp.arange(DEVICES, dtype=jnp.int32)
    onehot = (block_part[:, None] == number[None, :]).astype(jnp.float32)
    order = jnp.arange(BLOCKS, dtype=jnp.int32)
    before = lax.dot((order[:, None] > order[None, :]).astype(jnp.float32), onehot)
    rank = jnp.sum(onehot * before, axis=1).astype(jnp.int32)
    counts = counts.reshape(DEVICES, DEVICES)
    mine = jnp.sum(jnp.where(number[None, :] == me, counts, 0.0), axis=1)
    starts = lax.dot((number[:, None] > number[None, :]).astype(jnp.float32), mine).astype(jnp.int32)
    params = [row_params(v, d) for v, d in zip(values, (0.0, 1.0, 1.0, 0.0, 0.0))]
    per = 8
    served = pl.pallas_call(
        functools.partial(pack_kernel, per),
        grid=(DEVICES // per,),
        out_shape=jax.ShapeDtypeStruct((DEVICES, SLOTS * ROWS, LANES), jnp.float32),
        in_specs=[SCALARS, WHOLE] + [WHOLE] * 5,
        out_specs=pl.BlockSpec((per, SLOTS * ROWS, LANES), lambda i: (i, 0, 0)),
        compiler_params=pltpu.CompilerParams(vmem_limit_bytes=32 * 1024 * 1024),
    )(starts, states, *params)
    arrived = lax.all_to_all(served, AXES, split_axis=0, concat_axis=0, tiled=True)
    per = 16
    return pl.pallas_call(
        functools.partial(place_kernel, per),
        grid=(BLOCKS // per,),
        out_shape=jax.ShapeDtypeStruct((ROWS, BLOCKS * LANES), jnp.float32),
        in_specs=[SCALARS, WHOLE, pl.BlockSpec((per, LANES), lambda i: (i, 0))],
        out_specs=pl.BlockSpec((ROWS, per * LANES), lambda i: (0, i)),
        compiler_params=pltpu.CompilerParams(vmem_limit_bytes=32 * 1024 * 1024),
    )(block_part * SLOTS + rank, arrived, tile_perm)


def settle(parts, where, counts, states, block_part, tile_perm, *values):
    per = 16
    return pl.pallas_call(
        functools.partial(settle_kernel, per),
        grid=(BLOCKS // per,),
        out_shape=jax.ShapeDtypeStruct((ROWS, BLOCKS * LANES), jnp.float32),
        in_specs=[SCALARS, WHOLE, pl.BlockSpec((per, LANES), lambda i: (i, 0))],
        out_specs=pl.BlockSpec((ROWS, per * LANES), lambda i: (0, i)),
        compiler_params=pltpu.CompilerParams(vmem_limit_bytes=60 * 1024 * 1024),
    )(where, parts, tile_perm)


def on_device(states, block_part, tile_perm, *values):
    cap = LIMIT
    dma = pltpu.SemaphoreType.DMA
    parts, where, longest, counts = pl.pallas_call(
        functools.partial(move_kernel, cap),
        out_shape=(
            jax.ShapeDtypeStruct((2, 3, BLOCKS * PIECE, LANES), jnp.float32),
            jax.ShapeDtypeStruct((1, BLOCKS), jnp.int32),
            jax.ShapeDtypeStruct((1, 1), jnp.int32),
            jax.ShapeDtypeStruct((DEVICES, 1, DEVICES), jnp.float32),
        ),
        in_specs=[WHOLE, pl.BlockSpec(memory_space=pl.ANY)] + [WHOLE] * 5,
        out_specs=(WHOLE, WHOLE, SCALARS, WHOLE),
        scratch_shapes=[
            *[pltpu.VMEM((2 * BLOCKS * PIECE, LANES), jnp.float32)] * 3,
            *[pltpu.VMEM((4 * cap * PIECE, LANES), jnp.float32)] * 9,
            pltpu.VMEM((3, BLOCKS * PIECE, LANES), jnp.float32),
            pltpu.VMEM((3, 3, cap * PIECE, LANES), jnp.float32),
            pltpu.VMEM((ROWS, BLOCKS * LANES), jnp.float32),
            pltpu.VMEM((12, 4, 256), jnp.int32),
            *[pltpu.SMEM((4, 256), jnp.int32)] * 12,
            dma((CHUNKS,)), dma((12,)), dma((4, 3)), dma((4, 3)), dma((3, CHUNKS)), dma((3, CHUNKS)),
            dma((3, 3, 3)), dma((3, 3, 3)), dma((3,)), dma((3,)),
        ],
        compiler_params=pltpu.CompilerParams(collective_id=1, has_side_effects=True, vmem_limit_bytes=60 * 1024 * 1024),
    )(block_part.reshape(1, BLOCKS), states, *[v.reshape(1, ROWS - 1) for v in values])
    fits = longest[0, 0] <= cap
    return lax.cond(fits, settle, direct_route, parts, where.reshape(BLOCKS), counts, states, block_part, tile_perm, *values)


def solution(mesh):
    split = P(None, AXES)
    placed = (split, P(AXES), P(AXES, None), P(), P(), P(), P(), P())
    return jax.shard_map(on_device, mesh=mesh, in_specs=placed, out_specs=split, check_vma=False)
```

```python
import functools

import jax
import jax.numpy as jnp
from jax import lax
from jax.experimental import pallas as pl
from jax.experimental.pallas import tpu as pltpu
from jax.sharding import PartitionSpec as P

AXES = ("group", "peer")
DEVICES = 128
BLOCKS = 256
LANES = 128
ROWS = 41
SLOTS = 4
TIME_STEP = 0.25
PIECES = (4, 3)
HALF = 21
SETTLED = 24
LIMITS = (176, 184, 176)
SIZES = (4, 2, 4, 4)
STRIDES = (32, 16, 4, 1)
CORE = 1
ORDERS = ((3, 0, 2), (0, 2, 3), (2, 3, 0))
MESH = pl.DeviceIdType.MESH


def digits_of(device):
    return tuple(lax.rem(lax.div(device, st), n) for st, n in zip(STRIDES, SIZES))


def take_digits(number, dims):
    out = {}
    for d in reversed(dims):
        out[d] = number & (SIZES[d] - 1)
        number = number >> (SIZES[d].bit_length() - 1)
    return out, number


def cells(stage, order, own, r):
    if stage == 3:
        fixed_s, free_p, list_dim, held_by = tuple(order), (0, 1, 2, 3), CORE, order[2]
    else:
        fixed_s = tuple(order[:stage])
        free_p = tuple(sorted(fixed_s + (CORE,)))
        list_dim = order[stage]
        held_by = CORE if stage == 0 else order[stage - 1]
    free_s = tuple(d for d in range(4) if d not in fixed_s and d != list_dim)
    s, rest = take_digits(r, free_s)
    p, rest = take_digits(rest, free_p)
    s[list_dim] = rest
    slab = sum((s[d] if d in s else own[d]) * STRIDES[d] for d in range(4))
    part = sum((p[d] if d in p else own[d]) * STRIDES[d] for d in range(4))
    return slab, part, p[held_by]


def find_bases(stage, order, own, counts):
    col = lax.broadcasted_iota(jnp.int32, (256, 1), 0)
    row = lax.broadcasted_iota(jnp.int32, (1, 256), 1)
    slab, part, held = cells(stage, order, own, col)
    slab_r, part_r, held_r = cells(stage, order, own, row)
    device = lax.broadcasted_iota(jnp.int32, (1, DEVICES), 1)
    pick = (part == device).astype(jnp.float32)
    by_part = lax.dot_general(pick, counts, (((1,), (1,)), ((), ())), preferred_element_type=jnp.float32)
    n = jnp.sum(jnp.where(slab == device, by_part, 0.0), axis=1, keepdims=True)
    wide = jnp.broadcast_to(n, (256, LANES))
    earlier = (held_r == held) & (part_r * DEVICES + slab_r < part * DEVICES + slab)
    base = jnp.dot(earlier.astype(jnp.float32), wide, preferred_element_type=jnp.float32)[:, 0:1].astype(jnp.int32)
    return n, wide, base + held * (BLOCKS if stage == 0 else LIMITS[stage - 1])


def index_lists(stage, order, own, counts):
    size = 64
    n, wide, base = find_bases(stage, order, own, counts)
    col = lax.broadcasted_iota(jnp.int32, (256, 1), 0)
    row = lax.broadcasted_iota(jnp.int32, (1, 256), 1)
    ahead = ((row >> 6) == (col >> 6)) & (row < col)
    place = jnp.dot(ahead.astype(jnp.float32), wide, preferred_element_type=jnp.float32)[:, 0:1].astype(jnp.int32)
    end = place + n.astype(jnp.int32)
    gap = base - place
    limit = 2 * BLOCKS - 1 if stage == 0 else 4 * LIMITS[stage - 1] - 1
    out = []
    for k in range(4):
        one = slice(k * size, (k + 1) * size)
        inside = (row >= place[one]) & (row < end[one])
        found = row + jnp.sum(jnp.where(inside, gap[one], 0), axis=0, keepdims=True)
        out.append(jnp.clip(found, 0, limit))
    return out


def final_list(base, onehot, before):
    found = jnp.sum(onehot * (before + base.astype(jnp.float32)), axis=0, keepdims=True).astype(jnp.int32)
    return jnp.clip(found, 0, 4 * LIMITS[2] - 1)


def same_key(dims):
    i = lax.broadcasted_iota(jnp.int32, (DEVICES, DEVICES), 0)
    j = lax.broadcasted_iota(jnp.int32, (DEVICES, DEVICES), 1)
    mask = sum((SIZES[d] - 1) * STRIDES[d] for d in dims)
    return ((i & mask) == (j & mask)).astype(jnp.float32)


def excess_of_longest(counts):
    longest = None
    for order in ORDERS:
        for stage in range(3):
            to, left = order[:stage + 1], order[stage:]
            sums = jnp.dot(same_key(to), counts, preferred_element_type=jnp.float32)
            sums = jnp.dot(sums, same_key(left), preferred_element_type=jnp.float32)
            sums = sums - LIMITS[stage]
            longest = sums if longest is None else jnp.maximum(longest, sums)
    return jnp.max(longest, axis=0, keepdims=True)


def advance(block, half_volt, steepness, gate_rate, conductance, reversal):
    voltage = block[0:1, :]
    steady = jax.nn.sigmoid((voltage - half_volt) * steepness)
    damping = jnp.exp(-gate_rate * (1.0 + jax.nn.sigmoid(voltage)))
    gates = steady + (block - steady) * damping
    current = jnp.sum(conductance * gates * (voltage - reversal), axis=0, keepdims=True)
    row = lax.broadcasted_iota(jnp.int32, block.shape, 0)
    return jnp.where(row == 0, voltage - TIME_STEP * current, gates)


def column(values):
    lane = lax.broadcasted_iota(jnp.int32, (ROWS, ROWS - 1), 1)
    row = lax.broadcasted_iota(jnp.int32, (ROWS, ROWS - 1), 0)
    picked = jnp.sum(jnp.where(lane == row - 1, values, 0.0), axis=1, keepdims=True)
    return jnp.broadcast_to(picked, (ROWS, LANES))


CHUNKS = 4
CHUNK = BLOCKS // CHUNKS


def first_row(w, t):
    return t * PIECES[0] if w == 0 else 3 * PIECES[0] + t * PIECES[1]


def move_kernel(part_ref, states_ref, hv, st, gr, co, re, out_ref, longest_ref, counts_ref, *scratch):
    scratch = list(scratch)

    def take(count):
        taken = scratch[:count]
        del scratch[:count]
        return taken

    adv = [take(3) for w in range(2)]
    recv = [[take(3) for w in range(2)] for ph in range(3)]
    stage, send = take(2), take(2)
    states, tables = take(2)
    lists = take(12)
    settled, given, other_part = take(3)
    (load_sem, table_sem, count_send, count_recv, swap_send, swap_recv, send_sem, recv_sem,
     last_send, last_recv, part_send, part_recv, store_sem) = scratch
    me = lax.axis_index("group") * 16 + lax.axis_index("peer")
    own = digits_of(me)
    core = own[CORE]

    def at(coords):
        return (coords[0] * 2 + coords[CORE], coords[2] * 4 + coords[3])

    def along(dim, delta):
        to = lax.rem(own[dim] + delta, SIZES[dim])
        return at(tuple(to if d == dim else own[d] for d in range(4)))

    def load(k):
        columns = pl.ds(k * CHUNK * LANES, CHUNK * LANES)
        return pltpu.make_async_copy(states_ref.at[:, columns], states.at[:, columns], load_sem.at[k])

    for k in range(CHUNKS):
        load(k).start()
    barrier = pltpu.get_barrier_semaphore()
    neighbours = [(d, delta) for d in range(4) for delta in range(1, SIZES[d])]
    for d, delta in neighbours:
        pl.semaphore_signal(barrier, inc=1, device_id=along(d, delta), device_id_type=MESH)

    parts = part_ref[...]
    number = lax.broadcasted_iota(jnp.int32, (DEVICES, BLOCKS), 0)
    onehot = (number == parts).astype(jnp.float32)
    ones = jnp.ones((8, BLOCKS), jnp.float32)
    mine = lax.dot_general(ones, onehot, (((1,), (1,)), ((), ())), preferred_element_type=jnp.float32)[0:1]
    counts_ref[me] = mine
    params = [column(r[...]) for r in (hv, st, gr, co, re)]

    pl.semaphore_wait(barrier, len(neighbours))

    part_swap = pltpu.make_async_remote_copy(
        src_ref=part_ref, dst_ref=other_part, send_sem=part_send, recv_sem=part_recv,
        device_id=along(CORE, 1), device_id_type=MESH)
    part_swap.start()

    spread = (3, 2, 1, 0)

    def tell(k, delta):
        held = STRIDES[spread[k]]
        rows = pl.ds(lax.div(me, held) * held, held)
        return pltpu.make_async_remote_copy(
            src_ref=counts_ref.at[rows], dst_ref=counts_ref.at[rows],
            send_sem=count_send.at[k, delta - 1], recv_sem=count_recv.at[k, delta - 1],
            device_id=along(spread[k], delta), device_id_type=MESH)


    def update(i, carry):
        for u in range(8):
            b = i * 8 + u
            new = advance(states[:, pl.ds(pl.multiple_of(b * LANES, LANES), LANES)], *params)
            low = jnp.concatenate([new[0:16], new[32:37]], axis=0)
            high = jnp.concatenate([new[16:32], new[40:41], new[40:41], new[37:40]], axis=0)
            keep = jnp.where(core == 0, low, high)
            give = jnp.where(core == 0, high, low)
            for w, size in enumerate(PIECES):
                for t in range(3):
                    first = first_row(w, t)
                    adv[w][t][pl.ds((core * BLOCKS + b) * size, size), :] = keep[first:first + size]
                    stage[w][t, pl.ds(b * size, size), :] = give[first:first + size]
        return carry

    def swap(w, t, k):
        rows = CHUNK * PIECES[w]
        mine_at = core * (BLOCKS * PIECES[w])
        return pltpu.make_async_remote_copy(
            src_ref=stage[w].at[t, pl.ds(k * rows, rows)],
            dst_ref=adv[w][t].at[pl.ds(pl.multiple_of(mine_at + k * rows, 8), rows)],
            send_sem=swap_send.at[w, t, k], recv_sem=swap_recv.at[w, t, k],
            device_id=along(CORE, 1), device_id_type=MESH)

    for k in range(CHUNKS):
        for delta in range(1, SIZES[spread[k]]):
            tell(k, delta).start()
        load(k).wait()
        lax.fori_loop(k * CHUNK // 8, (k + 1) * CHUNK // 8, update, 0)
        for w in range(2):
            for t in range(3):
                swap(w, t, k).start()
        for delta in range(1, SIZES[spread[k]]):
            tell(k, delta).wait()

    counts = counts_ref[...].reshape(DEVICES, DEVICES)

    def table(ph, t):
        return pltpu.make_async_copy(tables.at[ph * 3 + t], lists[ph * 3 + t], table_sem.at[ph * 3 + t])

    def make_table(ph, t):
        for k, one in enumerate(index_lists(ph, ORDERS[t], own, counts)):
            tables[ph * 3 + t, k:k + 1, :] = one

    for t in range(3):
        make_table(0, t)
    for t in range(3):
        table(0, t).start()

    def hop(w, t, ph, delta):
        dim = ORDERS[t][ph]
        rows = LIMITS[ph] * PIECES[w]
        return pltpu.make_async_remote_copy(
            src_ref=send[w].at[t, delta - 1, pl.ds(0, rows)],
            dst_ref=recv[ph][w][t].at[pl.ds(pl.multiple_of(own[dim] * rows, 8), rows)],
            send_sem=send_sem.at[ph, w, t, delta - 1], recv_sem=recv_sem.at[ph, w, t, delta - 1],
            device_id=along(dim, delta), device_id_type=MESH)

    def gather(w, source, target, start, which, row, count):
        size = PIECES[w]

        def body(i, carry):
            for u in range(8):
                j = i * 8 + u
                target[pl.ds(start + j * size, size), :] = source[pl.ds(which[row, j] * size, size), :]
            return carry

        lax.fori_loop(0, count // 8, body, 0)

    def settle_piece(w, t, target, row, begin, end):
        size = PIECES[w]
        first = first_row(w, t)
        if first == HALF - size:
            first = first + size * core
        source, which = recv[2][w][t], lists[9 + t]

        def body(i, carry):
            for u in range(8):
                j = i * 8 + u
                target[j, pl.ds(first, size), :] = source[pl.ds(which[row, j] * size, size), :]
            return carry

        lax.fori_loop(begin // 8, end // 8, body, 0)

    def send_off(w, ph):
        sources = []
        for t in range(3):
            if ph == 0:
                for k in range(CHUNKS):
                    swap(w, t, k).wait()
                sources.append(adv[w][t])
            else:
                for delta in (2, 1, 3):
                    hop(w, t, ph - 1, delta).wait()
                sources.append(recv[ph - 1][w][t])
        for delta in (2, 1, 3, 0):
            for t in range(3):
                dim = ORDERS[t][ph]
                to = lax.rem(own[dim] + delta, 4)
                if delta:
                    gather(w, sources[t], send[w].at[t, delta - 1], 0, lists[ph * 3 + t], to, LIMITS[ph])
                    hop(w, t, ph, delta).start()
                else:
                    start = own[dim] * (LIMITS[ph] * PIECES[w])
                    gather(w, sources[t], recv[ph][w][t], start, lists[ph * 3 + t], to, LIMITS[ph])

    for ph in range(3):
        for t in range(3):
            table(ph, t).wait()
        for w in range(2):
            send_off(w, ph)
        if ph < 2:
            for t in range(3):
                make_table(ph + 1, t)
        else:
            part_swap.wait()
            theirs = (number == other_part[...]).astype(jnp.float32)
            r = lax.broadcasted_iota(jnp.int32, (BLOCKS, BLOCKS), 0)
            c = lax.broadcasted_iota(jnp.int32, (BLOCKS, BLOCKS), 1)
            earlier = (r < c).astype(jnp.float32)
            before = jnp.dot(onehot, earlier, preferred_element_type=jnp.float32)
            before_theirs = jnp.dot(theirs, earlier, preferred_element_type=jnp.float32)
            for t in range(3):
                base = find_bases(3, ORDERS[t], own, counts)[2]
                low, high = base[0:DEVICES], base[DEVICES:2 * DEVICES]
                tables[9 + t, 0:1, :] = final_list(jnp.where(core == 0, low, high), onehot, before)
                tables[9 + t, 1:2, :] = final_list(jnp.where(core == 0, high, low), theirs, before_theirs)
        for t in range(3):
            table(ph + 1, t).start()
        if ph == 0:
            longest_ref[0, 0] = jnp.max(excess_of_longest(counts)).astype(jnp.int32)

    pieces = ((0, BLOCKS, 0, 8), (0, BLOCKS // 2, 8, 16), (BLOCKS // 2, BLOCKS // 2, 8, 16))

    def last(k):
        b, n, r, m = pieces[k]
        return pltpu.make_async_remote_copy(
            src_ref=given.at[pl.ds(b, n), pl.ds(r, m)], dst_ref=out_ref.at[core, pl.ds(b, n), pl.ds(r, m)],
            send_sem=last_send.at[k], recv_sem=last_recv.at[k],
            device_id=along(CORE, 1), device_id_type=MESH)

    def store(k):
        b, n, r, m = pieces[k]
        return pltpu.make_async_copy(
            settled.at[pl.ds(b, n), pl.ds(r, m)], out_ref.at[core, pl.ds(b, n), pl.ds(r, m)], store_sem.at[k])

    for t in range(3):
        table(3, t).wait()
    for w in range(2):
        for t in range(3):
            for delta in (2, 1, 3):
                hop(w, t, 2, delta).wait()
        runs = ((0, 0, BLOCKS),) if w == 0 else ((1, 0, BLOCKS // 2), (2, BLOCKS // 2, BLOCKS))
        for target, row, copy in ((given, 1, last), (settled, 0, store)):
            for k, begin, end in runs:
                for t in range(3):
                    settle_piece(w, t, target, row, begin, end)
                copy(k).start()
    for k in range(3):
        last(k).wait()
        store(k).wait()


def settle_kernel(per_step, parts_ref, perm_ref, out_ref):
    early = lax.broadcasted_iota(jnp.int32, (8, LANES), 0) < 5
    for j in range(per_step):
        low, high = parts_ref[0, j], parts_ref[1, j]
        mixed = jnp.where(early, low[16:24], high[16:24])
        block = jnp.concatenate([low[0:16], high[0:16], mixed, high[16:17]], axis=0)
        index = jnp.broadcast_to(perm_ref[j:j + 1, :], (ROWS, LANES))
        out_ref[:, j * LANES:(j + 1) * LANES] = jnp.take_along_axis(block, index, axis=1)


def pack_kernel(per_step, starts_ref, states_ref, hv, st, gr, co, re, out_ref):
    step = pl.program_id(0)
    params = [r[...] for r in (hv, st, gr, co, re)]
    for j in range(per_step):
        first = starts_ref[step * per_step + j]
        for k in range(SLOTS):
            at = jnp.minimum(first + k, BLOCKS - 1)
            block = states_ref[:, pl.ds(pl.multiple_of(at * LANES, LANES), LANES)]
            out_ref[j, k * ROWS:(k + 1) * ROWS, :] = advance(block, *params)


def place_kernel(per_step, slots_ref, arrived_ref, perm_ref, out_ref):
    step = pl.program_id(0)
    for j in range(per_step):
        slot = slots_ref[step * per_step + j]
        part, rank = slot // SLOTS, slot % SLOTS
        block = arrived_ref[part, pl.ds(rank * ROWS, ROWS), :]
        index = jnp.broadcast_to(perm_ref[j:j + 1, :], (ROWS, LANES))
        out_ref[:, j * LANES:(j + 1) * LANES] = jnp.take_along_axis(block, index, axis=1)


def row_params(values, dummy):
    padded = jnp.concatenate([jnp.full((1,), dummy, values.dtype), values])
    return jnp.broadcast_to(padded[:, None], (ROWS, LANES))


WHOLE = pl.BlockSpec(memory_space=pltpu.VMEM)
SCALARS = pl.BlockSpec(memory_space=pltpu.SMEM)


def direct_route(parts, counts, states, block_part, tile_perm, *values):
    me = lax.axis_index(AXES)
    number = jnp.arange(DEVICES, dtype=jnp.int32)
    onehot = (block_part[:, None] == number[None, :]).astype(jnp.float32)
    order = jnp.arange(BLOCKS, dtype=jnp.int32)
    before = lax.dot((order[:, None] > order[None, :]).astype(jnp.float32), onehot)
    rank = jnp.sum(onehot * before, axis=1).astype(jnp.int32)
    counts = counts.reshape(DEVICES, DEVICES)
    mine = jnp.sum(jnp.where(number[None, :] == me, counts, 0.0), axis=1)
    starts = lax.dot((number[:, None] > number[None, :]).astype(jnp.float32), mine).astype(jnp.int32)
    params = [row_params(v, d) for v, d in zip(values, (0.0, 1.0, 1.0, 0.0, 0.0))]
    per = 8
    served = pl.pallas_call(
        functools.partial(pack_kernel, per),
        grid=(DEVICES // per,),
        out_shape=jax.ShapeDtypeStruct((DEVICES, SLOTS * ROWS, LANES), jnp.float32),
        in_specs=[SCALARS, WHOLE] + [WHOLE] * 5,
        out_specs=pl.BlockSpec((per, SLOTS * ROWS, LANES), lambda i: (i, 0, 0)),
        compiler_params=pltpu.CompilerParams(vmem_limit_bytes=32 * 1024 * 1024),
    )(starts, states, *params)
    arrived = lax.all_to_all(served, AXES, split_axis=0, concat_axis=0, tiled=True)
    per = 16
    return pl.pallas_call(
        functools.partial(place_kernel, per),
        grid=(BLOCKS // per,),
        out_shape=jax.ShapeDtypeStruct((ROWS, BLOCKS * LANES), jnp.float32),
        in_specs=[SCALARS, WHOLE, pl.BlockSpec((per, LANES), lambda i: (i, 0))],
        out_specs=pl.BlockSpec((ROWS, per * LANES), lambda i: (0, i)),
        compiler_params=pltpu.CompilerParams(vmem_limit_bytes=32 * 1024 * 1024),
    )(block_part * SLOTS + rank, arrived, tile_perm)


def settle(parts, counts, states, block_part, tile_perm, *values):
    per = 32
    return pl.pallas_call(
        functools.partial(settle_kernel, per),
        grid=(BLOCKS // per,),
        out_shape=jax.ShapeDtypeStruct((ROWS, BLOCKS * LANES), jnp.float32),
        in_specs=[
            pl.BlockSpec((2, per, SETTLED, LANES), lambda i: (0, i, 0, 0)),
            pl.BlockSpec((per, LANES), lambda i: (i, 0)),
        ],
        out_specs=pl.BlockSpec((ROWS, per * LANES), lambda i: (0, i)),
        compiler_params=pltpu.CompilerParams(vmem_limit_bytes=60 * 1024 * 1024),
    )(parts, tile_perm)


def on_device(states, block_part, tile_perm, *values):
    dma = pltpu.SemaphoreType.DMA
    parts, longest, counts = pl.pallas_call(
        move_kernel,
        out_shape=(
            jax.ShapeDtypeStruct((2, BLOCKS, SETTLED, LANES), jnp.float32),
            jax.ShapeDtypeStruct((1, 1), jnp.int32),
            jax.ShapeDtypeStruct((DEVICES, 1, DEVICES), jnp.float32),
        ),
        in_specs=[WHOLE, pl.BlockSpec(memory_space=pl.ANY)] + [WHOLE] * 5,
        out_specs=(pl.BlockSpec(memory_space=pl.ANY), SCALARS, WHOLE),
        scratch_shapes=[
            *[pltpu.VMEM((2 * BLOCKS * n, LANES), jnp.float32) for n in PIECES for t in range(3)],
            *[pltpu.VMEM((4 * limit * n, LANES), jnp.float32) for limit in LIMITS for n in PIECES for t in range(3)],
            *[pltpu.VMEM((3, BLOCKS * n, LANES), jnp.float32) for n in PIECES],
            *[pltpu.VMEM((3, 3, max(LIMITS) * n, LANES), jnp.float32) for n in PIECES],
            pltpu.VMEM((ROWS, BLOCKS * LANES), jnp.float32),
            pltpu.VMEM((12, 4, 256), jnp.int32),
            *[pltpu.SMEM((4, 256), jnp.int32)] * 12,
            pltpu.VMEM((BLOCKS, SETTLED, LANES), jnp.float32),
            pltpu.VMEM((BLOCKS, SETTLED, LANES), jnp.float32),
            pltpu.VMEM((1, BLOCKS), jnp.int32),
            dma((CHUNKS,)), dma((12,)), dma((4, 3)), dma((4, 3)), dma((2, 3, CHUNKS)), dma((2, 3, CHUNKS)),
            dma((3, 2, 3, 3)), dma((3, 2, 3, 3)), dma((3,)), dma((3,)), dma, dma, dma((3,)),
        ],
        compiler_params=pltpu.CompilerParams(collective_id=1, has_side_effects=True, vmem_limit_bytes=60 * 1024 * 1024),
    )(block_part.reshape(1, BLOCKS), states, *[v.reshape(1, ROWS - 1) for v in values])
    fits = longest[0, 0] <= 0
    return lax.cond(fits, settle, direct_route, parts, counts, states, block_part, tile_perm, *values)


def solution(mesh):
    split = P(None, AXES)
    placed = (split, P(AXES), P(AXES, None), P(), P(), P(), P(), P())
    return jax.shard_map(on_device, mesh=mesh, in_specs=placed, out_specs=split, check_vma=False)
```

```python
import functools

import jax
import jax.numpy as jnp
from jax import lax
from jax.experimental import pallas as pl
from jax.experimental.pallas import tpu as pltpu
from jax.sharding import PartitionSpec as P

AXES = ("group", "peer")
DEVICES = 128
BLOCKS = 256
LANES = 128
ROWS = 41
SLOTS = 4
TIME_STEP = 0.25
PIECES = (4, 3)
HALF = 21
SETTLED = 24
LIMITS = (176, 184, 176)
SIZES = (4, 2, 4, 4)
STRIDES = (32, 16, 4, 1)
CORE = 1
ORDERS = ((3, 0, 2), (0, 2, 3), (2, 3, 0))
MESH = pl.DeviceIdType.MESH


def digits_of(device):
    return tuple(lax.rem(lax.div(device, st), n) for st, n in zip(STRIDES, SIZES))


def take_digits(number, dims):
    out = {}
    for d in reversed(dims):
        out[d] = number & (SIZES[d] - 1)
        number = number >> (SIZES[d].bit_length() - 1)
    return out, number


def cells(stage, order, own, r):
    if stage == 3:
        fixed_s, free_p, list_dim, held_by = tuple(order), (0, 1, 2, 3), CORE, order[2]
    else:
        fixed_s = tuple(order[:stage])
        free_p = tuple(sorted(fixed_s + (CORE,)))
        list_dim = order[stage]
        held_by = CORE if stage == 0 else order[stage - 1]
    free_s = tuple(d for d in range(4) if d not in fixed_s and d != list_dim)
    s, rest = take_digits(r, free_s)
    p, rest = take_digits(rest, free_p)
    s[list_dim] = rest
    slab = sum((s[d] if d in s else own[d]) * STRIDES[d] for d in range(4))
    part = sum((p[d] if d in p else own[d]) * STRIDES[d] for d in range(4))
    return slab, part, p[held_by]


def find_bases(stage, order, own, counts):
    col = lax.broadcasted_iota(jnp.int32, (256, 1), 0)
    row = lax.broadcasted_iota(jnp.int32, (1, 256), 1)
    slab, part, held = cells(stage, order, own, col)
    slab_r, part_r, held_r = cells(stage, order, own, row)
    device = lax.broadcasted_iota(jnp.int32, (1, DEVICES), 1)
    pick = (part == device).astype(jnp.float32)
    by_part = lax.dot_general(pick, counts, (((1,), (1,)), ((), ())), preferred_element_type=jnp.float32)
    n = jnp.sum(jnp.where(slab == device, by_part, 0.0), axis=1, keepdims=True)
    wide = jnp.broadcast_to(n, (256, LANES))
    earlier = (held_r == held) & (part_r * DEVICES + slab_r < part * DEVICES + slab)
    base = jnp.dot(earlier.astype(jnp.float32), wide, preferred_element_type=jnp.float32)[:, 0:1].astype(jnp.int32)
    return n, wide, base + held * (BLOCKS if stage == 0 else LIMITS[stage - 1])


def index_lists(stage, order, own, counts):
    size = 64
    n, wide, base = find_bases(stage, order, own, counts)
    col = lax.broadcasted_iota(jnp.int32, (256, 1), 0)
    row = lax.broadcasted_iota(jnp.int32, (1, 256), 1)
    ahead = ((row >> 6) == (col >> 6)) & (row < col)
    place = jnp.dot(ahead.astype(jnp.float32), wide, preferred_element_type=jnp.float32)[:, 0:1].astype(jnp.int32)
    end = place + n.astype(jnp.int32)
    gap = base - place
    limit = 2 * BLOCKS - 1 if stage == 0 else 4 * LIMITS[stage - 1] - 1
    out = []
    for k in range(4):
        one = slice(k * size, (k + 1) * size)
        inside = (row >= place[one]) & (row < end[one])
        found = row + jnp.sum(jnp.where(inside, gap[one], 0), axis=0, keepdims=True)
        out.append(jnp.clip(found, 0, limit))
    return out


def final_list(base, onehot, before):
    found = jnp.sum(onehot * (before + base.astype(jnp.float32)), axis=0, keepdims=True).astype(jnp.int32)
    return jnp.clip(found, 0, 4 * LIMITS[2] - 1)


def same_key(dims):
    i = lax.broadcasted_iota(jnp.int32, (DEVICES, DEVICES), 0)
    j = lax.broadcasted_iota(jnp.int32, (DEVICES, DEVICES), 1)
    mask = sum((SIZES[d] - 1) * STRIDES[d] for d in dims)
    return ((i & mask) == (j & mask)).astype(jnp.float32)


def excess_of_longest(counts):
    longest = None
    for order in ORDERS:
        for stage in range(3):
            to, left = order[:stage + 1], order[stage:]
            sums = jnp.dot(same_key(to), counts, preferred_element_type=jnp.float32)
            sums = jnp.dot(sums, same_key(left), preferred_element_type=jnp.float32)
            sums = sums - LIMITS[stage]
            longest = sums if longest is None else jnp.maximum(longest, sums)
    return jnp.max(longest, axis=0, keepdims=True)


def advance(block, half_volt, steepness, gate_rate, conductance, reversal):
    voltage = block[0:1, :]
    steady = jax.nn.sigmoid((voltage - half_volt) * steepness)
    damping = jnp.exp(-gate_rate * (1.0 + jax.nn.sigmoid(voltage)))
    gates = steady + (block - steady) * damping
    current = jnp.sum(conductance * gates * (voltage - reversal), axis=0, keepdims=True)
    row = lax.broadcasted_iota(jnp.int32, block.shape, 0)
    return jnp.where(row == 0, voltage - TIME_STEP * current, gates)


def column(values):
    lane = lax.broadcasted_iota(jnp.int32, (ROWS, ROWS - 1), 1)
    row = lax.broadcasted_iota(jnp.int32, (ROWS, ROWS - 1), 0)
    picked = jnp.sum(jnp.where(lane == row - 1, values, 0.0), axis=1, keepdims=True)
    return jnp.broadcast_to(picked, (ROWS, LANES))


PLANE = [(0, 0, z, x) for z in range(4) for x in range(4) if z or x]
COLUMN = [(y, c, 0, 0) for y in range(4) for c in range(2) if y or c]
CHUNKS = 4
CHUNK = BLOCKS // CHUNKS


def first_row(w, t):
    return t * PIECES[0] if w == 0 else 3 * PIECES[0] + t * PIECES[1]


def move_kernel(part_ref, states_ref, hv, st, gr, co, re, out_ref, longest_ref, counts_ref, *scratch):
    scratch = list(scratch)

    def take(count):
        taken = scratch[:count]
        del scratch[:count]
        return taken

    adv = [take(3) for w in range(2)]
    recv = [[take(3) for w in range(2)] for ph in range(3)]
    stage, send = take(2), take(2)
    states, tables = take(2)
    lists = take(12)
    settled, given, other_part = take(3)
    (load_sem, table_sem, count_send, count_recv, swap_send, swap_recv, send_sem, recv_sem,
     last_send, last_recv, part_send, part_recv, store_sem) = scratch
    me = lax.axis_index("group") * 16 + lax.axis_index("peer")
    own = digits_of(me)
    core = own[CORE]

    def at(coords):
        return (coords[0] * 2 + coords[CORE], coords[2] * 4 + coords[3])

    def shifted(shift):
        return at(tuple(lax.rem(own[d] + shift[d], SIZES[d]) if shift[d] else own[d] for d in range(4)))

    def along(dim, delta):
        return shifted(tuple(delta if d == dim else 0 for d in range(4)))

    def load(k):
        columns = pl.ds(k * CHUNK * LANES, CHUNK * LANES)
        return pltpu.make_async_copy(states_ref.at[:, columns], states.at[:, columns], load_sem.at[k])

    for k in range(CHUNKS):
        load(k).start()
    barrier = pltpu.get_barrier_semaphore()
    for shift in PLANE + COLUMN:
        pl.semaphore_signal(barrier, inc=1, device_id=shifted(shift), device_id_type=MESH)

    parts = part_ref[...]
    number = lax.broadcasted_iota(jnp.int32, (DEVICES, BLOCKS), 0)
    onehot = (number == parts).astype(jnp.float32)
    ones = jnp.ones((8, BLOCKS), jnp.float32)
    mine = lax.dot_general(ones, onehot, (((1,), (1,)), ((), ())), preferred_element_type=jnp.float32)[0:1]
    counts_ref[me] = mine
    params = [column(r[...]) for r in (hv, st, gr, co, re)]

    pl.semaphore_wait(barrier, len(PLANE) + len(COLUMN))

    part_swap = pltpu.make_async_remote_copy(
        src_ref=part_ref, dst_ref=other_part, send_sem=part_send, recv_sem=part_recv,
        device_id=along(CORE, 1), device_id_type=MESH)
    part_swap.start()

    def tell(k, i):
        held = 16 if k else 1
        rows = pl.ds(lax.div(me, held) * held, held)
        return pltpu.make_async_remote_copy(
            src_ref=counts_ref.at[rows], dst_ref=counts_ref.at[rows],
            send_sem=count_send.at[k, i], recv_sem=count_recv.at[k, i],
            device_id=shifted((PLANE, COLUMN)[k][i]), device_id_type=MESH)

    def update(i, carry):
        for u in range(8):
            b = i * 8 + u
            new = advance(states[:, pl.ds(pl.multiple_of(b * LANES, LANES), LANES)], *params)
            low = jnp.concatenate([new[0:16], new[32:37]], axis=0)
            high = jnp.concatenate([new[16:32], new[40:41], new[40:41], new[37:40]], axis=0)
            keep = jnp.where(core == 0, low, high)
            give = jnp.where(core == 0, high, low)
            for w, size in enumerate(PIECES):
                for t in range(3):
                    first = first_row(w, t)
                    adv[w][t][pl.ds((core * BLOCKS + b) * size, size), :] = keep[first:first + size]
                    stage[w][t, pl.ds(b * size, size), :] = give[first:first + size]
        return carry

    def swap(w, t, k):
        rows = CHUNK * PIECES[w]
        mine_at = core * (BLOCKS * PIECES[w])
        return pltpu.make_async_remote_copy(
            src_ref=stage[w].at[t, pl.ds(k * rows, rows)],
            dst_ref=adv[w][t].at[pl.ds(pl.multiple_of(mine_at + k * rows, 8), rows)],
            send_sem=swap_send.at[w, t, k], recv_sem=swap_recv.at[w, t, k],
            device_id=along(CORE, 1), device_id_type=MESH)

    for k in range(CHUNKS):
        if k == 0:
            for i in range(len(PLANE)):
                tell(0, i).start()
        if k == CHUNKS - 1:
            for i in range(len(PLANE)):
                tell(0, i).wait()
            for i in range(len(COLUMN)):
                tell(1, i).start()
        load(k).wait()
        lax.fori_loop(k * CHUNK // 8, (k + 1) * CHUNK // 8, update, 0)
        for w in range(2):
            for t in range(3):
                swap(w, t, k).start()
    for i in range(len(COLUMN)):
        tell(1, i).wait()

    counts = counts_ref[...].reshape(DEVICES, DEVICES)

    def table(ph, t):
        return pltpu.make_async_copy(tables.at[ph * 3 + t], lists[ph * 3 + t], table_sem.at[ph * 3 + t])

    def make_table(ph, t):
        for k, one in enumerate(index_lists(ph, ORDERS[t], own, counts)):
            tables[ph * 3 + t, k:k + 1, :] = one

    for t in range(3):
        make_table(0, t)
        table(0, t).start()

    def hop(w, t, ph, delta):
        dim = ORDERS[t][ph]
        rows = LIMITS[ph] * PIECES[w]
        return pltpu.make_async_remote_copy(
            src_ref=send[w].at[t, delta - 1, pl.ds(0, rows)],
            dst_ref=recv[ph][w][t].at[pl.ds(pl.multiple_of(own[dim] * rows, 8), rows)],
            send_sem=send_sem.at[ph, w, t, delta - 1], recv_sem=recv_sem.at[ph, w, t, delta - 1],
            device_id=along(dim, delta), device_id_type=MESH)

    def gather(w, source, target, start, which, row, count):
        size = PIECES[w]

        def body(i, carry):
            for u in range(8):
                j = i * 8 + u
                target[pl.ds(start + j * size, size), :] = source[pl.ds(which[row, j] * size, size), :]
            return carry

        lax.fori_loop(0, count // 8, body, 0)

    def settle_piece(w, t, target, row, begin, end):
        size = PIECES[w]
        first = first_row(w, t)
        if first == HALF - size:
            first = first + size * core
        source, which = recv[2][w][t], lists[9 + t]

        def body(i, carry):
            for u in range(8):
                j = i * 8 + u
                target[j, pl.ds(first, size), :] = source[pl.ds(which[row, j] * size, size), :]
            return carry

        lax.fori_loop(begin // 8, end // 8, body, 0)

    def send_off(w, ph):
        sources = []
        for t in range(3):
            if ph == 0:
                for k in range(CHUNKS):
                    swap(w, t, k).wait()
                sources.append(adv[w][t])
            else:
                for delta in (2, 1, 3):
                    hop(w, t, ph - 1, delta).wait()
                sources.append(recv[ph - 1][w][t])
        for delta in (2, 1, 3, 0):
            for t in range(3):
                dim = ORDERS[t][ph]
                to = lax.rem(own[dim] + delta, 4)
                if delta:
                    gather(w, sources[t], send[w].at[t, delta - 1], 0, lists[ph * 3 + t], to, LIMITS[ph])
                    hop(w, t, ph, delta).start()
                else:
                    start = own[dim] * (LIMITS[ph] * PIECES[w])
                    gather(w, sources[t], recv[ph][w][t], start, lists[ph * 3 + t], to, LIMITS[ph])

    for ph in range(3):
        for t in range(3):
            table(ph, t).wait()
        for w in range(2):
            send_off(w, ph)
        if ph < 2:
            for t in range(3):
                make_table(ph + 1, t)
        else:
            part_swap.wait()
            theirs = (number == other_part[...]).astype(jnp.float32)
            r = lax.broadcasted_iota(jnp.int32, (BLOCKS, BLOCKS), 0)
            c = lax.broadcasted_iota(jnp.int32, (BLOCKS, BLOCKS), 1)
            earlier = (r < c).astype(jnp.float32)
            before = jnp.dot(onehot, earlier, preferred_element_type=jnp.float32)
            before_theirs = jnp.dot(theirs, earlier, preferred_element_type=jnp.float32)
            for t in range(3):
                base = find_bases(3, ORDERS[t], own, counts)[2]
                low, high = base[0:DEVICES], base[DEVICES:2 * DEVICES]
                tables[9 + t, 0:1, :] = final_list(jnp.where(core == 0, low, high), onehot, before)
                tables[9 + t, 1:2, :] = final_list(jnp.where(core == 0, high, low), theirs, before_theirs)
        for t in range(3):
            table(ph + 1, t).start()
        if ph == 0:
            longest_ref[0, 0] = jnp.max(excess_of_longest(counts)).astype(jnp.int32)

    pieces = ((0, BLOCKS, 0, 8), (0, BLOCKS // 2, 8, 16), (BLOCKS // 2, BLOCKS // 2, 8, 16))

    def last(k):
        b, n, r, m = pieces[k]
        return pltpu.make_async_remote_copy(
            src_ref=given.at[pl.ds(b, n), pl.ds(r, m)], dst_ref=out_ref.at[core, pl.ds(b, n), pl.ds(r, m)],
            send_sem=last_send.at[k], recv_sem=last_recv.at[k],
            device_id=along(CORE, 1), device_id_type=MESH)

    def store(k):
        b, n, r, m = pieces[k]
        return pltpu.make_async_copy(
            settled.at[pl.ds(b, n), pl.ds(r, m)], out_ref.at[core, pl.ds(b, n), pl.ds(r, m)], store_sem.at[k])

    for t in range(3):
        table(3, t).wait()
    for w in range(2):
        for t in range(3):
            for delta in (2, 1, 3):
                hop(w, t, 2, delta).wait()
        runs = ((0, 0, BLOCKS),) if w == 0 else ((1, 0, BLOCKS // 2), (2, BLOCKS // 2, BLOCKS))
        for target, row, copy in ((given, 1, last), (settled, 0, store)):
            for k, begin, end in runs:
                for t in range(3):
                    settle_piece(w, t, target, row, begin, end)
                copy(k).start()
    for k in range(3):
        last(k).wait()
        store(k).wait()


def settle_kernel(per_step, parts_ref, perm_ref, out_ref):
    early = lax.broadcasted_iota(jnp.int32, (8, LANES), 0) < 5
    for j in range(per_step):
        low, high = parts_ref[0, j], parts_ref[1, j]
        mixed = jnp.where(early, low[16:24], high[16:24])
        block = jnp.concatenate([low[0:16], high[0:16], mixed, high[16:17]], axis=0)
        index = jnp.broadcast_to(perm_ref[j:j + 1, :], (ROWS, LANES))
        out_ref[:, j * LANES:(j + 1) * LANES] = jnp.take_along_axis(block, index, axis=1)


def pack_kernel(per_step, starts_ref, states_ref, hv, st, gr, co, re, out_ref):
    step = pl.program_id(0)
    params = [r[...] for r in (hv, st, gr, co, re)]
    for j in range(per_step):
        first = starts_ref[step * per_step + j]
        for k in range(SLOTS):
            at = jnp.minimum(first + k, BLOCKS - 1)
            block = states_ref[:, pl.ds(pl.multiple_of(at * LANES, LANES), LANES)]
            out_ref[j, k * ROWS:(k + 1) * ROWS, :] = advance(block, *params)


def place_kernel(per_step, slots_ref, arrived_ref, perm_ref, out_ref):
    step = pl.program_id(0)
    for j in range(per_step):
        slot = slots_ref[step * per_step + j]
        part, rank = slot // SLOTS, slot % SLOTS
        block = arrived_ref[part, pl.ds(rank * ROWS, ROWS), :]
        index = jnp.broadcast_to(perm_ref[j:j + 1, :], (ROWS, LANES))
        out_ref[:, j * LANES:(j + 1) * LANES] = jnp.take_along_axis(block, index, axis=1)


def row_params(values, dummy):
    padded = jnp.concatenate([jnp.full((1,), dummy, values.dtype), values])
    return jnp.broadcast_to(padded[:, None], (ROWS, LANES))


WHOLE = pl.BlockSpec(memory_space=pltpu.VMEM)
SCALARS = pl.BlockSpec(memory_space=pltpu.SMEM)


def direct_route(parts, counts, states, block_part, tile_perm, *values):
    me = lax.axis_index(AXES)
    number = jnp.arange(DEVICES, dtype=jnp.int32)
    onehot = (block_part[:, None] == number[None, :]).astype(jnp.float32)
    order = jnp.arange(BLOCKS, dtype=jnp.int32)
    before = lax.dot((order[:, None] > order[None, :]).astype(jnp.float32), onehot)
    rank = jnp.sum(onehot * before, axis=1).astype(jnp.int32)
    counts = counts.reshape(DEVICES, DEVICES)
    mine = jnp.sum(jnp.where(number[None, :] == me, counts, 0.0), axis=1)
    starts = lax.dot((number[:, None] > number[None, :]).astype(jnp.float32), mine).astype(jnp.int32)
    params = [row_params(v, d) for v, d in zip(values, (0.0, 1.0, 1.0, 0.0, 0.0))]
    per = 8
    served = pl.pallas_call(
        functools.partial(pack_kernel, per),
        grid=(DEVICES // per,),
        out_shape=jax.ShapeDtypeStruct((DEVICES, SLOTS * ROWS, LANES), jnp.float32),
        in_specs=[SCALARS, WHOLE] + [WHOLE] * 5,
        out_specs=pl.BlockSpec((per, SLOTS * ROWS, LANES), lambda i: (i, 0, 0)),
        compiler_params=pltpu.CompilerParams(vmem_limit_bytes=32 * 1024 * 1024),
    )(starts, states, *params)
    arrived = lax.all_to_all(served, AXES, split_axis=0, concat_axis=0, tiled=True)
    per = 16
    return pl.pallas_call(
        functools.partial(place_kernel, per),
        grid=(BLOCKS // per,),
        out_shape=jax.ShapeDtypeStruct((ROWS, BLOCKS * LANES), jnp.float32),
        in_specs=[SCALARS, WHOLE, pl.BlockSpec((per, LANES), lambda i: (i, 0))],
        out_specs=pl.BlockSpec((ROWS, per * LANES), lambda i: (0, i)),
        compiler_params=pltpu.CompilerParams(vmem_limit_bytes=32 * 1024 * 1024),
    )(block_part * SLOTS + rank, arrived, tile_perm)


def settle(parts, counts, states, block_part, tile_perm, *values):
    per = 128
    return pl.pallas_call(
        functools.partial(settle_kernel, per),
        grid=(BLOCKS // per,),
        out_shape=jax.ShapeDtypeStruct((ROWS, BLOCKS * LANES), jnp.float32),
        in_specs=[
            pl.BlockSpec((2, per, SETTLED, LANES), lambda i: (0, i, 0, 0)),
            pl.BlockSpec((per, LANES), lambda i: (i, 0)),
        ],
        out_specs=pl.BlockSpec((ROWS, per * LANES), lambda i: (0, i)),
        compiler_params=pltpu.CompilerParams(vmem_limit_bytes=60 * 1024 * 1024),
    )(parts, tile_perm)


def on_device(states, block_part, tile_perm, *values):
    dma = pltpu.SemaphoreType.DMA
    parts, longest, counts = pl.pallas_call(
        move_kernel,
        out_shape=(
            jax.ShapeDtypeStruct((2, BLOCKS, SETTLED, LANES), jnp.float32),
            jax.ShapeDtypeStruct((1, 1), jnp.int32),
            jax.ShapeDtypeStruct((DEVICES, 1, DEVICES), jnp.float32),
        ),
        in_specs=[WHOLE, pl.BlockSpec(memory_space=pl.ANY)] + [WHOLE] * 5,
        out_specs=(pl.BlockSpec(memory_space=pl.ANY), SCALARS, WHOLE),
        scratch_shapes=[
            *[pltpu.VMEM((2 * BLOCKS * n, LANES), jnp.float32) for n in PIECES for t in range(3)],
            *[pltpu.VMEM((4 * limit * n, LANES), jnp.float32) for limit in LIMITS for n in PIECES for t in range(3)],
            *[pltpu.VMEM((3, BLOCKS * n, LANES), jnp.float32) for n in PIECES],
            *[pltpu.VMEM((3, 3, max(LIMITS) * n, LANES), jnp.float32) for n in PIECES],
            pltpu.VMEM((ROWS, BLOCKS * LANES), jnp.float32),
            pltpu.VMEM((12, 4, 256), jnp.int32),
            *[pltpu.SMEM((4, 256), jnp.int32)] * 12,
            pltpu.VMEM((BLOCKS, SETTLED, LANES), jnp.float32),
            pltpu.VMEM((BLOCKS, SETTLED, LANES), jnp.float32),
            pltpu.VMEM((1, BLOCKS), jnp.int32),
            dma((CHUNKS,)), dma((12,)), dma((2, 15)), dma((2, 15)), dma((2, 3, CHUNKS)), dma((2, 3, CHUNKS)),
            dma((3, 2, 3, 3)), dma((3, 2, 3, 3)), dma((3,)), dma((3,)), dma, dma, dma((3,)),
        ],
        compiler_params=pltpu.CompilerParams(collective_id=1, has_side_effects=True, vmem_limit_bytes=60 * 1024 * 1024),
    )(block_part.reshape(1, BLOCKS), states, *[v.reshape(1, ROWS - 1) for v in values])
    fits = longest[0, 0] <= 0
    return lax.cond(fits, settle, direct_route, parts, counts, states, block_part, tile_perm, *values)


def solution(mesh):
    split = P(None, AXES)
    placed = (split, P(AXES), P(AXES, None), P(), P(), P(), P(), P())
    return jax.shard_map(on_device, mesh=mesh, in_specs=placed, out_specs=split, check_vma=False)
```

```python
import functools

import jax
import jax.numpy as jnp
from jax import lax
from jax.experimental import pallas as pl
from jax.experimental.pallas import tpu as pltpu
from jax.sharding import PartitionSpec as P

AXES = ("group", "peer")
DEVICES = 128
BLOCKS = 256
LANES = 128
ROWS = 41
SLOTS = 4
TIME_STEP = 0.25
PIECES = (4, 3)
HALF = 21
SETTLED = 24
LIMITS = (176, 184, 176)
SIZES = (4, 2, 4, 4)
STRIDES = (32, 16, 4, 1)
CORE = 1
ORDERS = ((3, 0, 2), (0, 2, 3), (2, 3, 0))
MESH = pl.DeviceIdType.MESH


def digits_of(device):
    return tuple(lax.rem(lax.div(device, st), n) for st, n in zip(STRIDES, SIZES))


def take_digits(number, dims):
    out = {}
    for d in reversed(dims):
        out[d] = number & (SIZES[d] - 1)
        number = number >> (SIZES[d].bit_length() - 1)
    return out, number


def cells(stage, order, own, r):
    if stage == 3:
        fixed_s, free_p, list_dim, held_by = tuple(order), (0, 1, 2, 3), CORE, order[2]
    else:
        fixed_s = tuple(order[:stage])
        free_p = tuple(sorted(fixed_s + (CORE,)))
        list_dim = order[stage]
        held_by = CORE if stage == 0 else order[stage - 1]
    free_s = tuple(d for d in range(4) if d not in fixed_s and d != list_dim)
    s, rest = take_digits(r, free_s)
    p, rest = take_digits(rest, free_p)
    s[list_dim] = rest
    slab = sum((s[d] if d in s else own[d]) * STRIDES[d] for d in range(4))
    part = sum((p[d] if d in p else own[d]) * STRIDES[d] for d in range(4))
    return slab, part, p[held_by]


def find_bases(stage, order, own, counts):
    col = lax.broadcasted_iota(jnp.int32, (256, 1), 0)
    row = lax.broadcasted_iota(jnp.int32, (1, 256), 1)
    slab, part, held = cells(stage, order, own, col)
    slab_r, part_r, held_r = cells(stage, order, own, row)
    device = lax.broadcasted_iota(jnp.int32, (1, DEVICES), 1)
    pick = (part == device).astype(jnp.float32)
    by_part = lax.dot_general(pick, counts, (((1,), (1,)), ((), ())), preferred_element_type=jnp.float32)
    n = jnp.sum(jnp.where(slab == device, by_part, 0.0), axis=1, keepdims=True)
    wide = jnp.broadcast_to(n, (256, LANES))
    earlier = (held_r == held) & (part_r * DEVICES + slab_r < part * DEVICES + slab)
    base = jnp.dot(earlier.astype(jnp.float32), wide, preferred_element_type=jnp.float32)[:, 0:1].astype(jnp.int32)
    return n, wide, base + held * (BLOCKS if stage == 0 else LIMITS[stage - 1])


def index_lists(stage, order, own, counts):
    size = 64
    n, wide, base = find_bases(stage, order, own, counts)
    col = lax.broadcasted_iota(jnp.int32, (256, 1), 0)
    row = lax.broadcasted_iota(jnp.int32, (1, 256), 1)
    ahead = ((row >> 6) == (col >> 6)) & (row < col)
    place = jnp.dot(ahead.astype(jnp.float32), wide, preferred_element_type=jnp.float32)[:, 0:1].astype(jnp.int32)
    end = place + n.astype(jnp.int32)
    gap = base - place
    limit = 2 * BLOCKS - 1 if stage == 0 else 4 * LIMITS[stage - 1] - 1
    out = []
    for k in range(4):
        one = slice(k * size, (k + 1) * size)
        inside = (row >= place[one]) & (row < end[one])
        found = row + jnp.sum(jnp.where(inside, gap[one], 0), axis=0, keepdims=True)
        out.append(jnp.clip(found, 0, limit))
    return out


def final_list(base, onehot, before):
    found = jnp.sum(onehot * (before + base.astype(jnp.float32)), axis=0, keepdims=True).astype(jnp.int32)
    return jnp.clip(found, 0, 4 * LIMITS[2] - 1)


def same_key(dims):
    i = lax.broadcasted_iota(jnp.int32, (DEVICES, DEVICES), 0)
    j = lax.broadcasted_iota(jnp.int32, (DEVICES, DEVICES), 1)
    mask = sum((SIZES[d] - 1) * STRIDES[d] for d in dims)
    return ((i & mask) == (j & mask)).astype(jnp.float32)


def excess_of_longest(counts):
    longest = None
    for order in ORDERS:
        for stage in range(3):
            to, left = order[:stage + 1], order[stage:]
            sums = jnp.dot(same_key(to), counts, preferred_element_type=jnp.float32)
            sums = jnp.dot(sums, same_key(left), preferred_element_type=jnp.float32)
            sums = sums - LIMITS[stage]
            longest = sums if longest is None else jnp.maximum(longest, sums)
    return jnp.max(longest, axis=0, keepdims=True)


def advance(block, half_volt, steepness, gate_rate, conductance, reversal):
    voltage = block[0:1, :]
    steady = jax.nn.sigmoid((voltage - half_volt) * steepness)
    damping = jnp.exp(-gate_rate * (1.0 + jax.nn.sigmoid(voltage)))
    gates = steady + (block - steady) * damping
    current = jnp.sum(conductance * gates * (voltage - reversal), axis=0, keepdims=True)
    row = lax.broadcasted_iota(jnp.int32, block.shape, 0)
    return jnp.where(row == 0, voltage - TIME_STEP * current, gates)


def column(values):
    lane = lax.broadcasted_iota(jnp.int32, (ROWS, ROWS - 1), 1)
    row = lax.broadcasted_iota(jnp.int32, (ROWS, ROWS - 1), 0)
    picked = jnp.sum(jnp.where(lane == row - 1, values, 0.0), axis=1, keepdims=True)
    return jnp.broadcast_to(picked, (ROWS, LANES))


PLANE = [(0, 0, z, x) for z in range(4) for x in range(4) if z or x]
COLUMN = [(y, c, 0, 0) for y in range(4) for c in range(2) if y or c]
CHUNKS = 4
CHUNK = BLOCKS // CHUNKS


def first_row(w, t):
    return t * PIECES[0] if w == 0 else 3 * PIECES[0] + t * PIECES[1]


def move_kernel(part_ref, states_ref, hv, st, gr, co, re, out_ref, longest_ref, counts_ref, *scratch):
    scratch = list(scratch)

    def take(count):
        taken = scratch[:count]
        del scratch[:count]
        return taken

    adv = [take(3) for w in range(2)]
    recv = [[take(3) for w in range(2)] for ph in range(3)]
    stage, send = take(2), take(2)
    states, tables = take(2)
    lists = take(12)
    settled, given, other_part = take(3)
    (load_sem, table_sem, count_send, count_recv, swap_send, swap_recv, send_sem, recv_sem,
     last_send, last_recv, part_send, part_recv, store_sem) = scratch
    me = lax.axis_index("group") * 16 + lax.axis_index("peer")
    own = digits_of(me)
    core = own[CORE]

    def at(coords):
        return (coords[0] * 2 + coords[CORE], coords[2] * 4 + coords[3])

    def shifted(shift):
        return at(tuple(lax.rem(own[d] + shift[d], SIZES[d]) if shift[d] else own[d] for d in range(4)))

    def along(dim, delta):
        return shifted(tuple(delta if d == dim else 0 for d in range(4)))

    def load(k):
        columns = pl.ds(k * CHUNK * LANES, CHUNK * LANES)
        return pltpu.make_async_copy(states_ref.at[:, columns], states.at[:, columns], load_sem.at[k])

    for k in range(CHUNKS):
        load(k).start()
    barrier = pltpu.get_barrier_semaphore()
    for shift in PLANE + COLUMN:
        pl.semaphore_signal(barrier, inc=1, device_id=shifted(shift), device_id_type=MESH)

    parts = part_ref[...]
    number = lax.broadcasted_iota(jnp.int32, (DEVICES, BLOCKS), 0)
    onehot = (number == parts).astype(jnp.float32)
    ones = jnp.ones((8, BLOCKS), jnp.float32)
    mine = lax.dot_general(ones, onehot, (((1,), (1,)), ((), ())), preferred_element_type=jnp.float32)[0:1]
    counts_ref[me] = mine
    params = [column(r[...]) for r in (hv, st, gr, co, re)]

    pl.semaphore_wait(barrier, len(PLANE) + len(COLUMN))

    part_swap = pltpu.make_async_remote_copy(
        src_ref=part_ref, dst_ref=other_part, send_sem=part_send, recv_sem=part_recv,
        device_id=along(CORE, 1), device_id_type=MESH)
    part_swap.start()

    def tell(k, i):
        held = 16 if k else 1
        rows = pl.ds(lax.div(me, held) * held, held)
        return pltpu.make_async_remote_copy(
            src_ref=counts_ref.at[rows], dst_ref=counts_ref.at[rows],
            send_sem=count_send.at[k, i], recv_sem=count_recv.at[k, i],
            device_id=shifted((PLANE, COLUMN)[k][i]), device_id_type=MESH)

    def update(i, carry):
        for u in range(8):
            b = i * 8 + u
            new = advance(states[:, pl.ds(pl.multiple_of(b * LANES, LANES), LANES)], *params)
            low = jnp.concatenate([new[0:16], new[32:37]], axis=0)
            high = jnp.concatenate([new[16:32], new[40:41], new[40:41], new[37:40]], axis=0)
            keep = jnp.where(core == 0, low, high)
            give = jnp.where(core == 0, high, low)
            for w, size in enumerate(PIECES):
                for t in range(3):
                    first = first_row(w, t)
                    adv[w][t][pl.ds((core * BLOCKS + b) * size, size), :] = keep[first:first + size]
                    stage[w][t, pl.ds(b * size, size), :] = give[first:first + size]
        return carry

    def swap(w, t, k):
        rows = CHUNK * PIECES[w]
        mine_at = core * (BLOCKS * PIECES[w])
        return pltpu.make_async_remote_copy(
            src_ref=stage[w].at[t, pl.ds(k * rows, rows)],
            dst_ref=adv[w][t].at[pl.ds(pl.multiple_of(mine_at + k * rows, 8), rows)],
            send_sem=swap_send.at[w, t, k], recv_sem=swap_recv.at[w, t, k],
            device_id=along(CORE, 1), device_id_type=MESH)

    for k in range(CHUNKS):
        if k == 0:
            for i in range(len(PLANE)):
                tell(0, i).start()
        if k == CHUNKS - 1:
            for i in range(len(PLANE)):
                tell(0, i).wait()
            for i in range(len(COLUMN)):
                tell(1, i).start()
        load(k).wait()
        lax.fori_loop(k * CHUNK // 8, (k + 1) * CHUNK // 8, update, 0)
        for w in range(2):
            for t in range(3):
                swap(w, t, k).start()
    for i in range(len(COLUMN)):
        tell(1, i).wait()

    counts = counts_ref[...].reshape(DEVICES, DEVICES)

    def table(ph, t):
        return pltpu.make_async_copy(tables.at[ph * 3 + t], lists[ph * 3 + t], table_sem.at[ph * 3 + t])

    def make_table(ph, t):
        for k, one in enumerate(index_lists(ph, ORDERS[t], own, counts)):
            tables[ph * 3 + t, k:k + 1, :] = one

    for t in range(3):
        make_table(0, t)
        table(0, t).start()

    def hop(w, t, ph, delta):
        dim = ORDERS[t][ph]
        rows = LIMITS[ph] * PIECES[w]
        return pltpu.make_async_remote_copy(
            src_ref=send[w].at[t, delta - 1, pl.ds(0, rows)],
            dst_ref=recv[ph][w][t].at[pl.ds(pl.multiple_of(own[dim] * rows, 8), rows)],
            send_sem=send_sem.at[ph, w, t, delta - 1], recv_sem=recv_sem.at[ph, w, t, delta - 1],
            device_id=along(dim, delta), device_id_type=MESH)

    def gather(w, source, target, start, which, row, count):
        size = PIECES[w]
        step = 16 if count % 16 == 0 else 8

        def body(i, carry):
            for u in range(step):
                j = i * step + u
                target[pl.ds(start + j * size, size), :] = source[pl.ds(which[row, j] * size, size), :]
            return carry

        lax.fori_loop(0, count // step, body, 0)

    def settle_piece(w, t, target, row, begin, end):
        size = PIECES[w]
        first = first_row(w, t)
        if first == HALF - size:
            first = first + size * core
        source, which = recv[2][w][t], lists[9 + t]

        def body(i, carry):
            for u in range(8):
                j = i * 8 + u
                target[j, pl.ds(first, size), :] = source[pl.ds(which[row, j] * size, size), :]
            return carry

        lax.fori_loop(begin // 8, end // 8, body, 0)

    def send_off(w, ph):
        sources = []
        for t in range(3):
            if ph == 0:
                for k in range(CHUNKS):
                    swap(w, t, k).wait()
                sources.append(adv[w][t])
            else:
                for delta in (2, 1, 3):
                    hop(w, t, ph - 1, delta).wait()
                sources.append(recv[ph - 1][w][t])
        for delta in (2, 1, 3, 0):
            for t in range(3):
                dim = ORDERS[t][ph]
                to = lax.rem(own[dim] + delta, 4)
                if delta:
                    gather(w, sources[t], send[w].at[t, delta - 1], 0, lists[ph * 3 + t], to, LIMITS[ph])
                    hop(w, t, ph, delta).start()
                else:
                    start = own[dim] * (LIMITS[ph] * PIECES[w])
                    gather(w, sources[t], recv[ph][w][t], start, lists[ph * 3 + t], to, LIMITS[ph])

    for ph in range(3):
        for t in range(3):
            table(ph, t).wait()
        for w in range(2):
            send_off(w, ph)
        if ph < 2:
            for t in range(3):
                make_table(ph + 1, t)
        else:
            part_swap.wait()
            theirs = (number == other_part[...]).astype(jnp.float32)
            r = lax.broadcasted_iota(jnp.int32, (BLOCKS, BLOCKS), 0)
            c = lax.broadcasted_iota(jnp.int32, (BLOCKS, BLOCKS), 1)
            earlier = (r < c).astype(jnp.float32)
            before = jnp.dot(onehot, earlier, preferred_element_type=jnp.float32)
            before_theirs = jnp.dot(theirs, earlier, preferred_element_type=jnp.float32)
            for t in range(3):
                base = find_bases(3, ORDERS[t], own, counts)[2]
                low, high = base[0:DEVICES], base[DEVICES:2 * DEVICES]
                tables[9 + t, 0:1, :] = final_list(jnp.where(core == 0, low, high), onehot, before)
                tables[9 + t, 1:2, :] = final_list(jnp.where(core == 0, high, low), theirs, before_theirs)
        for t in range(3):
            table(ph + 1, t).start()
        if ph == 0:
            longest_ref[0, 0] = jnp.max(excess_of_longest(counts)).astype(jnp.int32)

    pieces = ((0, BLOCKS, 0, 12), (0, BLOCKS // 2, 12, 12), (BLOCKS // 2, BLOCKS // 2, 12, 12))

    def last(k):
        b, n, r, m = pieces[k]
        return pltpu.make_async_remote_copy(
            src_ref=given.at[pl.ds(b, n), pl.ds(r, m)], dst_ref=out_ref.at[core, pl.ds(b, n), pl.ds(r, m)],
            send_sem=last_send.at[k], recv_sem=last_recv.at[k],
            device_id=along(CORE, 1), device_id_type=MESH)

    def store(k):
        b, n, r, m = pieces[k]
        return pltpu.make_async_copy(
            settled.at[pl.ds(b, n), pl.ds(r, m)], out_ref.at[core, pl.ds(b, n), pl.ds(r, m)], store_sem.at[k])

    for t in range(3):
        table(3, t).wait()
    for w in range(2):
        for t in range(3):
            for delta in (2, 1, 3):
                hop(w, t, 2, delta).wait()
        runs = ((0, 0, BLOCKS),) if w == 0 else ((1, 0, BLOCKS // 2), (2, BLOCKS // 2, BLOCKS))
        for target, row, copy in ((given, 1, last), (settled, 0, store)):
            for k, begin, end in runs:
                for t in range(3):
                    settle_piece(w, t, target, row, begin, end)
                copy(k).start()
    for k in range(3):
        last(k).wait()
        store(k).wait()


def settle_kernel(per_step, parts_ref, perm_ref, out_ref):
    early = lax.broadcasted_iota(jnp.int32, (8, LANES), 0) < 5
    for j in range(per_step):
        low, high = parts_ref[0, j], parts_ref[1, j]
        mixed = jnp.where(early, low[16:24], high[16:24])
        block = jnp.concatenate([low[0:16], high[0:16], mixed, high[16:17]], axis=0)
        index = jnp.broadcast_to(perm_ref[j:j + 1, :], (ROWS, LANES))
        out_ref[:, j * LANES:(j + 1) * LANES] = jnp.take_along_axis(block, index, axis=1)


def pack_kernel(per_step, starts_ref, states_ref, hv, st, gr, co, re, out_ref):
    step = pl.program_id(0)
    params = [r[...] for r in (hv, st, gr, co, re)]
    for j in range(per_step):
        first = starts_ref[step * per_step + j]
        for k in range(SLOTS):
            at = jnp.minimum(first + k, BLOCKS - 1)
            block = states_ref[:, pl.ds(pl.multiple_of(at * LANES, LANES), LANES)]
            out_ref[j, k * ROWS:(k + 1) * ROWS, :] = advance(block, *params)


def place_kernel(per_step, slots_ref, arrived_ref, perm_ref, out_ref):
    step = pl.program_id(0)
    for j in range(per_step):
        slot = slots_ref[step * per_step + j]
        part, rank = slot // SLOTS, slot % SLOTS
        block = arrived_ref[part, pl.ds(rank * ROWS, ROWS), :]
        index = jnp.broadcast_to(perm_ref[j:j + 1, :], (ROWS, LANES))
        out_ref[:, j * LANES:(j + 1) * LANES] = jnp.take_along_axis(block, index, axis=1)


def row_params(values, dummy):
    padded = jnp.concatenate([jnp.full((1,), dummy, values.dtype), values])
    return jnp.broadcast_to(padded[:, None], (ROWS, LANES))


WHOLE = pl.BlockSpec(memory_space=pltpu.VMEM)
SCALARS = pl.BlockSpec(memory_space=pltpu.SMEM)


def direct_route(parts, counts, states, block_part, tile_perm, *values):
    me = lax.axis_index(AXES)
    number = jnp.arange(DEVICES, dtype=jnp.int32)
    onehot = (block_part[:, None] == number[None, :]).astype(jnp.float32)
    order = jnp.arange(BLOCKS, dtype=jnp.int32)
    before = lax.dot((order[:, None] > order[None, :]).astype(jnp.float32), onehot)
    rank = jnp.sum(onehot * before, axis=1).astype(jnp.int32)
    counts = counts.reshape(DEVICES, DEVICES)
    mine = jnp.sum(jnp.where(number[None, :] == me, counts, 0.0), axis=1)
    starts = lax.dot((number[:, None] > number[None, :]).astype(jnp.float32), mine).astype(jnp.int32)
    params = [row_params(v, d) for v, d in zip(values, (0.0, 1.0, 1.0, 0.0, 0.0))]
    per = 8
    served = pl.pallas_call(
        functools.partial(pack_kernel, per),
        grid=(DEVICES // per,),
        out_shape=jax.ShapeDtypeStruct((DEVICES, SLOTS * ROWS, LANES), jnp.float32),
        in_specs=[SCALARS, WHOLE] + [WHOLE] * 5,
        out_specs=pl.BlockSpec((per, SLOTS * ROWS, LANES), lambda i: (i, 0, 0)),
        compiler_params=pltpu.CompilerParams(vmem_limit_bytes=32 * 1024 * 1024),
    )(starts, states, *params)
    arrived = lax.all_to_all(served, AXES, split_axis=0, concat_axis=0, tiled=True)
    per = 16
    return pl.pallas_call(
        functools.partial(place_kernel, per),
        grid=(BLOCKS // per,),
        out_shape=jax.ShapeDtypeStruct((ROWS, BLOCKS * LANES), jnp.float32),
        in_specs=[SCALARS, WHOLE, pl.BlockSpec((per, LANES), lambda i: (i, 0))],
        out_specs=pl.BlockSpec((ROWS, per * LANES), lambda i: (0, i)),
        compiler_params=pltpu.CompilerParams(vmem_limit_bytes=32 * 1024 * 1024),
    )(block_part * SLOTS + rank, arrived, tile_perm)


def settle(parts, counts, states, block_part, tile_perm, *values):
    per = 128
    return pl.pallas_call(
        functools.partial(settle_kernel, per),
        grid=(BLOCKS // per,),
        out_shape=jax.ShapeDtypeStruct((ROWS, BLOCKS * LANES), jnp.float32),
        in_specs=[
            pl.BlockSpec((2, per, SETTLED, LANES), lambda i: (0, i, 0, 0)),
            pl.BlockSpec((per, LANES), lambda i: (i, 0)),
        ],
        out_specs=pl.BlockSpec((ROWS, per * LANES), lambda i: (0, i)),
        compiler_params=pltpu.CompilerParams(vmem_limit_bytes=60 * 1024 * 1024),
    )(parts, tile_perm)


def on_device(states, block_part, tile_perm, *values):
    dma = pltpu.SemaphoreType.DMA
    parts, longest, counts = pl.pallas_call(
        move_kernel,
        out_shape=(
            jax.ShapeDtypeStruct((2, BLOCKS, SETTLED, LANES), jnp.float32),
            jax.ShapeDtypeStruct((1, 1), jnp.int32),
            jax.ShapeDtypeStruct((DEVICES, 1, DEVICES), jnp.float32),
        ),
        in_specs=[WHOLE, pl.BlockSpec(memory_space=pl.ANY)] + [WHOLE] * 5,
        out_specs=(pl.BlockSpec(memory_space=pl.ANY), SCALARS, WHOLE),
        scratch_shapes=[
            *[pltpu.VMEM((2 * BLOCKS * n, LANES), jnp.float32) for n in PIECES for t in range(3)],
            *[pltpu.VMEM((4 * limit * n, LANES), jnp.float32) for limit in LIMITS for n in PIECES for t in range(3)],
            *[pltpu.VMEM((3, BLOCKS * n, LANES), jnp.float32) for n in PIECES],
            *[pltpu.VMEM((3, 3, max(LIMITS) * n, LANES), jnp.float32) for n in PIECES],
            pltpu.VMEM((ROWS, BLOCKS * LANES), jnp.float32),
            pltpu.VMEM((12, 4, 256), jnp.int32),
            *[pltpu.SMEM((4, 256), jnp.int32)] * 12,
            pltpu.VMEM((BLOCKS, SETTLED, LANES), jnp.float32),
            pltpu.VMEM((BLOCKS, SETTLED, LANES), jnp.float32),
            pltpu.VMEM((1, BLOCKS), jnp.int32),
            dma((CHUNKS,)), dma((12,)), dma((2, 15)), dma((2, 15)), dma((2, 3, CHUNKS)), dma((2, 3, CHUNKS)),
            dma((3, 2, 3, 3)), dma((3, 2, 3, 3)), dma((3,)), dma((3,)), dma, dma, dma((3,)),
        ],
        compiler_params=pltpu.CompilerParams(collective_id=1, has_side_effects=True, vmem_limit_bytes=60 * 1024 * 1024),
    )(block_part.reshape(1, BLOCKS), states, *[v.reshape(1, ROWS - 1) for v in values])
    fits = longest[0, 0] <= 0
    return lax.cond(fits, settle, direct_route, parts, counts, states, block_part, tile_perm, *values)


def solution(mesh):
    split = P(None, AXES)
    placed = (split, P(AXES), P(AXES, None), P(), P(), P(), P(), P())
    return jax.shard_map(on_device, mesh=mesh, in_specs=placed, out_specs=split, check_vma=False)
```
